128 devices in a mesh: batch: 8 (over x_lo, y), mp: 16 (over x_hi, z, core).
Axes of the slice: x: 4 (x_hi: 2, x_lo: 2; x = x_hi * 2 + x_lo), y: 4, z: 4, core: 2. Of those that a mesh axis runs over, the one named last changes fastest.
Arguments:
- pixels: bfloat16 [8, 16, 8, 100, 768], P('batch', 'mp'), may hold values from -6 to 6
- patch_weight: bfloat16 [768, 1024], P('mp'), may hold values from -0.21875 to 0.21875
- position: bfloat16 [100, 1024], replicated, may hold values from -3 to 3
- encoder_gains: float32 [3, 1024], replicated, may hold values from 0.25 to 1.75
- qkv_weight: bfloat16 [1024, 3072], P('mp'), may hold values from -0.1875 to 0.1875
- out_weight: bfloat16 [1024, 1024], P('mp'), may hold values from -0.1875 to 0.1875
- up_weight: bfloat16 [1024, 4096], P('mp'), may hold values from -0.1875 to 0.1875
- down_weight: bfloat16 [4096, 1024], P('mp'), may hold values from -0.09375 to 0.09375
- cond_weight: bfloat16 [1024, 512], replicated, may hold values from -0.1875 to 0.1875
- time_weight: float32 [512, 512], replicated, may hold values from -0.5 to 0.5
- action_in: float32 [10, 512], replicated, may hold values from -2 to 2
- action_pos: float32 [16, 512], replicated, may hold values from -3 to 3
- denoise_gains: float32 [3, 512], replicated, may hold values from 0.25 to 1.75
- self_qkv: bfloat16 [512, 1536], replicated, may hold values from -0.25 to 0.25
- self_out: bfloat16 [512, 512], replicated, may hold values from -0.25 to 0.25
- cross_query: bfloat16 [512, 512], replicated, may hold values from -0.25 to 0.25
- cross_kv: bfloat16 [512, 1024], replicated, may hold values from -0.25 to 0.25
- cross_out: bfloat16 [512, 512], replicated, may hold values from -0.25 to 0.25
- mix_up: bfloat16 [512, 2048], replicated, may hold values from -0.25 to 0.25
- mix_down: bfloat16 [2048, 512], replicated, may hold values from -0.125 to 0.125
- action_out: float32 [512, 10], replicated, may hold values from -0.25 to 0.25
- noise: float32 [16, 8, 8, 16, 10], P('mp', 'batch'), may hold values from -5 to 5
- timesteps: int32 [4], replicated, may hold values from 5 to 79, as said below
Outputs:
- actions: float32 [16, 8, 8, 16, 10], P('mp', 'batch')
The draws below stay inside these ranges and needn't reach their ends.
Inputs may be any that keep to these rules, and one draw needn't show every extreme that they name: `timesteps`: strictly decreasing.
All inputs are finite; a program needn't handle non-finite values.
Results may differ from the reference program's by a relative error of at most 0.0033.
Values may be sent and summed in bfloat16 or wider, within the bound.
A program may use at most 192 MiB of HBM per device.

```python
import math
import jax
import jax.numpy as jnp
from jax import lax

D = 1024
HEADS = 16
FF = 4096
GRID = 10
PATCH_PIX = 768
VIEWS = 8
W = 512
DHEADS = 8
DFF = 2048
CAND = 8
SPAN = 16
ACT = 10
STEPS = 4
TMAX = 100
HEAD_DIM = 64
PATCHES = 100
CELLS = 25
DHEAD = 64
GROUPS = 16
BLOCK = 8


def draw_timesteps(key, part):
    order = jax.random.permutation(key, TMAX - 27)
    middle = jnp.sort(order[:STEPS - 2] + 6)[::-1]
    top = jnp.full((1,), TMAX - 21, jnp.int32)
    bottom = jnp.full((1,), 5, jnp.int32)
    return jnp.concatenate([top, middle.astype(jnp.int32), bottom]).astype(jnp.int32)


def block_levels(own_key, dims, shards, least, top_value):
    level, own = 1.0, jax.random.fold_in(own_key, 6)
    for dim, blocks in shards:
        steps = jnp.exp(jax.random.uniform(jax.random.fold_in(own, dim), (blocks,), jnp.float32, least / len(shards), top_value / len(shards)))
        level = level * jnp.repeat(steps, dims[dim] // blocks).reshape([-1 if axis == dim else 1 for axis in range(len(dims))])
    return level


def normal_values(stream_key, shape, scale, most, shards=(), held_as=jnp.bfloat16):
    entries = jax.random.normal(stream_key, shape, jnp.float32) * scale
    if len(shards) > 0:
        entries = block_levels(stream_key, shape, shards, -0.22, 0.18) * entries
    return jnp.clip(entries, min=-most, max=most).astype(held_as)


def setup_inputs(seed: int = 0) -> dict:
    streams_of = jax.random.split(jax.random.key(seed), 24)
    pixels = normal_values(streams_of[0], (VIEWS, GROUPS, BLOCK, PATCHES, PATCH_PIX), 1.0, 6.0, ((0, 8), (1, 16)))
    patch_weight = normal_values(streams_of[1], (PATCH_PIX, D), PATCH_PIX ** -0.5, 0.21875, ((0, 16),))
    position = normal_values(streams_of[2], (PATCHES, D), 0.5, 3.0)
    encoder_gains = jnp.clip(1.0 + 0.15 * jax.random.normal(streams_of[3], (3, D), jnp.float32), 0.25, 1.75)
    qkv_weight = normal_values(streams_of[4], (D, 3 * D), D ** -0.5, 0.1875, ((0, 16),))
    out_weight = normal_values(streams_of[5], (D, D), D ** -0.5, 0.1875, ((0, 16),))
    up_weight = normal_values(streams_of[6], (D, FF), D ** -0.5, 0.1875, ((0, 16),))
    down_weight = normal_values(streams_of[7], (FF, D), FF ** -0.5, 0.09375, ((0, 16),))
    cond_weight = normal_values(streams_of[8], (D, W), D ** -0.5, 0.1875)
    time_weight = normal_values(streams_of[9], (W, W), (W // 4) ** -0.5, 0.5, (), jnp.float32)
    action_in = normal_values(streams_of[10], (ACT, W), ACT ** -0.5, 2.0, (), jnp.float32)
    action_pos = normal_values(streams_of[11], (SPAN, W), 0.5, 3.0, (), jnp.float32)
    denoise_gains = jnp.clip(1.0 + 0.15 * jax.random.normal(streams_of[12], (3, W), jnp.float32), 0.25, 1.75)
    self_qkv = normal_values(streams_of[13], (W, 3 * W), W ** -0.5, 0.25)
    self_out = normal_values(streams_of[14], (W, W), W ** -0.5, 0.25)
    cross_query = normal_values(streams_of[15], (W, W), W ** -0.5, 0.25)
    cross_kv = normal_values(streams_of[16], (W, 2 * W), W ** -0.5, 0.25)
    cross_out = normal_values(streams_of[17], (W, W), W ** -0.5, 0.25)
    mix_up = normal_values(streams_of[18], (W, DFF), W ** -0.5, 0.25)
    mix_down = normal_values(streams_of[19], (DFF, W), DFF ** -0.5, 0.125)
    action_out = normal_values(streams_of[20], (W, ACT), W ** -0.5, 0.25, (), jnp.float32)
    noise = normal_values(streams_of[21], (GROUPS, BLOCK, CAND, SPAN, ACT), 1.0, 5.0, ((0, 16), (1, 8)), jnp.float32)
    timesteps = draw_timesteps(jax.random.fold_in(streams_of[23], 71), 0)
    return {"pixels": pixels, "patch_weight": patch_weight, "position": position, "encoder_gains": encoder_gains, "qkv_weight": qkv_weight, "out_weight": out_weight, "up_weight": up_weight, "down_weight": down_weight, "cond_weight": cond_weight, "time_weight": time_weight, "action_in": action_in, "action_pos": action_pos, "denoise_gains": denoise_gains, "self_qkv": self_qkv, "self_out": self_out, "cross_query": cross_query, "cross_kv": cross_kv, "cross_out": cross_out, "mix_up": mix_up, "mix_down": mix_down, "action_out": action_out, "noise": noise, "timesteps": timesteps}


norm_eps = 1e-06
offset = 0.008

def normalize(values, gain):
    middle = lax.optimization_barrier(jnp.mean(values, -1, keepdims=True))
    centred = values - middle
    spread = lax.optimization_barrier(jnp.mean(centred * centred, -1, keepdims=True))
    return centred * lax.rsqrt(spread + norm_eps) * gain

def plan(level):
    angle = (level.astype(jnp.float32) / TMAX + offset) / (1.0 + offset) * (math.pi / 2)
    base = math.cos(offset / (1.0 + offset) * math.pi / 2) ** 2
    return jnp.cos(angle) ** 2 / base

def product(left, right):
    return jnp.dot(left, right, preferred_element_type=jnp.float32)

def precise(left, right):
    return jnp.dot(left, right, precision=lax.Precision.HIGHEST)

def encode(frames, patch_weight, position, encoder_gains, qkv_weight, out_weight, up_weight, down_weight):
    count = frames.shape[0]
    state = product(frames.reshape(-1, PATCH_PIX), patch_weight).reshape(count, PATCHES, D)
    state = state + position.astype(jnp.float32)
    normed = normalize(state, encoder_gains[0]).astype(jnp.bfloat16).reshape(-1, D)
    packed = product(normed, qkv_weight).astype(jnp.bfloat16).reshape(count, PATCHES, 3, HEADS, HEAD_DIM)
    query = packed[:, :, 0].astype(jnp.float32)
    keys = packed[:, :, 1].astype(jnp.float32)
    values = packed[:, :, 2].astype(jnp.float32)
    scores = jnp.einsum('nqhd,nkhd->nhqk', query, keys) / math.sqrt(HEAD_DIM)
    probs = jax.nn.softmax(scores, -1).astype(jnp.bfloat16)
    context = jnp.einsum('nhqk,nkhd->nqhd', probs.astype(jnp.float32), values).astype(jnp.bfloat16)
    state = state + product(context.reshape(-1, D), out_weight).reshape(count, PATCHES, D)
    normed = normalize(state, encoder_gains[1]).astype(jnp.bfloat16).reshape(-1, D)
    hidden = jax.nn.gelu(product(normed, up_weight), approximate=False).astype(jnp.bfloat16)
    state = state + product(hidden, down_weight).reshape(count, PATCHES, D)
    final = normalize(state, encoder_gains[2]).reshape(count, GRID // 2, 2, GRID // 2, 2, D)
    return lax.optimization_barrier(jnp.mean(final, axis=(2, 4))).reshape(count, CELLS, D).astype(jnp.bfloat16)

def predict(sample, level, memory, params):
    time_weight, action_in, action_pos, gains, self_qkv, self_out, cross_query, cross_out, mix_up, mix_down, action_out = params
    samples = sample.shape[0]
    half = W // 2
    freqs = jnp.exp(-math.log(10000.0) * jnp.arange(half, dtype=jnp.float32) / half)
    phase = level.astype(jnp.float32) * freqs
    stamp = precise(jnp.concatenate([jnp.sin(phase), jnp.cos(phase)])[None, :], time_weight)[0]
    state = precise(sample.reshape(-1, ACT), action_in).reshape(samples, CAND, SPAN, W) + action_pos + stamp
    normed = normalize(state, gains[0]).astype(jnp.bfloat16).reshape(-1, W)
    packed = product(normed, self_qkv).astype(jnp.bfloat16).reshape(samples, CAND, SPAN, 3, DHEADS, DHEAD)
    query = packed[:, :, :, 0].astype(jnp.float32)
    keys = packed[:, :, :, 1].astype(jnp.float32)
    values = packed[:, :, :, 2].astype(jnp.float32)
    scores = jnp.einsum('sctgd,scugd->scgtu', query, keys) / math.sqrt(DHEAD)
    probs = jax.nn.softmax(scores, -1).astype(jnp.bfloat16)
    context = jnp.einsum('scgtu,scugd->sctgd', probs.astype(jnp.float32), values).astype(jnp.bfloat16)
    state = state + product(context.reshape(-1, W), self_out).reshape(state.shape)
    normed = normalize(state, gains[1]).astype(jnp.bfloat16).reshape(-1, W)
    asked = product(normed, cross_query).astype(jnp.bfloat16).reshape(samples, CAND * SPAN, DHEADS, DHEAD)
    length = memory.shape[1]
    far_keys = memory[:, :, :W].reshape(samples, length, DHEADS, DHEAD).astype(jnp.float32)
    far_values = memory[:, :, W:].reshape(samples, length, DHEADS, DHEAD).astype(jnp.float32)
    scores = jnp.einsum('sqgd,skgd->sgqk', asked.astype(jnp.float32), far_keys) / math.sqrt(DHEAD)
    probs = jax.nn.softmax(scores, -1).astype(jnp.bfloat16)
    context = jnp.einsum('sgqk,skgd->sqgd', probs.astype(jnp.float32), far_values).astype(jnp.bfloat16)
    state = state + product(context.reshape(-1, W), cross_out).reshape(state.shape)
    normed = normalize(state, gains[2]).astype(jnp.bfloat16).reshape(-1, W)
    hidden = jax.nn.gelu(product(normed, mix_up), approximate=False).astype(jnp.bfloat16)
    state = state + product(hidden, mix_down).reshape(state.shape)
    return precise(state.reshape(-1, W), action_out).reshape(sample.shape)

def reference(pixels, patch_weight, position, encoder_gains, qkv_weight, out_weight, up_weight, down_weight, cond_weight, time_weight, action_in, action_pos, denoise_gains, self_qkv, self_out, cross_query, cross_kv, cross_out, mix_up, mix_down, action_out, noise, timesteps):
    blocks = pixels.reshape(VIEWS * GROUPS, BLOCK, PATCHES, PATCH_PIX)

    def encode_block(frames):
        return encode(frames, patch_weight, position, encoder_gains, qkv_weight, out_weight, up_weight, down_weight)
    pooled = lax.map(encode_block, blocks)
    condition = product(pooled.reshape(-1, D), cond_weight).astype(jnp.bfloat16)
    memory = product(condition, cross_kv).astype(jnp.bfloat16)
    memory = memory.reshape(VIEWS, GROUPS, BLOCK, CELLS, 2 * W)
    memory = jnp.transpose(memory, (1, 2, 0, 3, 4)).reshape(GROUPS * BLOCK, VIEWS * CELLS, 2 * W)
    params = (time_weight, action_in, action_pos, denoise_gains, self_qkv, self_out, cross_query, cross_out, mix_up, mix_down, action_out)
    sample = noise.reshape(GROUPS * BLOCK, CAND, SPAN, ACT)
    for step in range(STEPS):
        level = timesteps[step]
        current = plan(level)
        if step + 1 < STEPS:
            after = plan(timesteps[step + 1])
        else:
            after = jnp.ones((), jnp.float32)
        predicted = predict(sample, level, memory, params)
        clean = (sample - jnp.sqrt(1.0 - current) * predicted) / jnp.sqrt(current)
        sample = jnp.sqrt(after) * clean + jnp.sqrt(1.0 - after) * predicted
    return sample.reshape(noise.shape)
```

```python
import math

import jax
import jax.numpy as jnp
from jax import lax
from jax.experimental import pallas as pl
from jax.experimental.pallas import tpu as pltpu
from jax.sharding import PartitionSpec as P

HEADS = 16
GRID = 10
DHEADS = 8
STEPS = 4
TMAX = 100


norm_eps = 1e-06
offset = 0.008


def in_one_piece(arrays, axis, dim, along):
    widths = [a.shape[along] for a in arrays]
    both = jnp.concatenate(arrays, axis=along)
    result = lax.all_gather(both, axis, axis=dim, tiled=True)
    return tuple(jnp.split(result, [sum(widths[:k]) for k in range(1, len(widths))], axis=along))


def normalize(values, gain):
    middle = jnp.mean(values, -1, keepdims=True)
    centred = values - middle
    spread = jnp.mean(centred * centred, -1, keepdims=True)
    return centred * lax.rsqrt(spread + norm_eps) * gain


def plan(level):
    angle = (level.astype(jnp.float32) / TMAX + offset) / (1.0 + offset) * (math.pi / 2)
    base = math.cos(offset / (1.0 + offset) * math.pi / 2) ** 2
    return jnp.cos(angle) ** 2 / base


def product(left, right):
    return jnp.dot(left, right, preferred_element_type=jnp.float32)


def precise(left, right):
    return jnp.dot(left, right, precision=lax.Precision.HIGHEST)


def contract(form, left, right):
    return jnp.einsum(form, left, right, preferred_element_type=jnp.float32)


VMEM = pltpu.VMEM
KEYS = 32


def stacked_heads(block):
    lane = lax.broadcasted_iota(jnp.int32, block.shape, 1)
    low = jnp.where(lane < 64, block, jnp.zeros_like(block))
    high = jnp.where(lane < 64, jnp.zeros_like(block), block)
    return jnp.concatenate([low, high], axis=0)


def pair_attention(query, keys, values, allowed):
    rows = query.shape[0]
    scores = lax.dot_general(
        stacked_heads(query), keys, (((1,), (1,)), ((), ())), preferred_element_type=jnp.float32
    )
    scores = jnp.where(allowed, scores * 0.125, -1e30)
    top = jnp.max(scores, axis=-1, keepdims=True)
    grown = jnp.exp(scores - top)
    probs = (grown / jnp.sum(grown, axis=-1, keepdims=True)).astype(jnp.bfloat16)
    both = jnp.dot(probs, values, preferred_element_type=jnp.float32)
    lane = lax.broadcasted_iota(jnp.int32, (rows, 128), 1)
    return jnp.where(lane < 64, both[:rows], both[rows:]).astype(jnp.bfloat16)


def gelu(values):
    return 0.5 * values * (1.0 + lax.erf(values * math.sqrt(0.5)))


def denoise_kernel(
    levels_ref,
    noise_ref,
    condition_ref,
    time_ref,
    in_ref,
    pos_ref,
    gains_ref,
    qkv_ref,
    self_out_ref,
    query_ref,
    kv_ref,
    cross_out_ref,
    up_ref,
    down_ref,
    out_ref,
    actions_ref,
    memory,
    stamps,
    packed,
    context,
):
    width = 512
    rows = 128
    memory[...] = product(condition_ref[...], kv_ref[...]).astype(jnp.bfloat16)
    row = lax.broadcasted_iota(jnp.int32, (8, width // 2), 0)
    level = jnp.zeros((8, width // 2), jnp.float32)
    for step in range(STEPS):
        level = jnp.where(row == step, levels_ref[step].astype(jnp.float32), level)
    order = lax.broadcasted_iota(jnp.int32, (8, width // 2), 1).astype(jnp.float32)
    phase = level * jnp.exp(order * (-math.log(10000.0) / (width // 2)))
    waves = jnp.concatenate([jnp.sin(phase), jnp.cos(phase)], axis=1)
    stamps[...] = precise(waves, time_ref[...])
    actions_ref[...] = noise_ref[...]

    own = lax.broadcasted_iota(jnp.int32, (2 * rows, rows), 0)
    other = lax.broadcasted_iota(jnp.int32, (2 * rows, rows), 1)
    same = lax.rem(own, rows) // 16 == other // 16
    slot = lax.broadcasted_iota(jnp.int32, (2 * rows, 8 * KEYS), 1)
    held = lax.rem(slot, KEYS) < 25

    def one_step(step, carry):
        sample = actions_ref[...]
        state = precise(sample, in_ref[...])
        state = (state.reshape(8, 16, width) + pos_ref[...]).reshape(rows, width)
        state = state + stamps[pl.ds(step, 1), :]
        normed = normalize(state, gains_ref[0:1, :]).astype(jnp.bfloat16)
        packed[...] = product(normed, qkv_ref[...]).astype(jnp.bfloat16)
        for pair in range(4):
            at = pair * 128
            context[:, at : at + 128] = pair_attention(
                packed[:, at : at + 128],
                packed[:, width + at : width + at + 128],
                packed[:, 2 * width + at : 2 * width + at + 128],
                same,
            )
        state = state + product(context[...], self_out_ref[...])
        normed = normalize(state, gains_ref[1:2, :]).astype(jnp.bfloat16)
        packed[:, 0:width] = product(normed, query_ref[...]).astype(jnp.bfloat16)
        for pair in range(4):
            at = pair * 128
            context[:, at : at + 128] = pair_attention(
                packed[:, at : at + 128],
                memory[:, at : at + 128],
                memory[:, width + at : width + at + 128],
                held,
            )
        state = state + product(context[...], cross_out_ref[...])
        normed = normalize(state, gains_ref[2:3, :]).astype(jnp.bfloat16)
        hidden = gelu(product(normed, up_ref[...])).astype(jnp.bfloat16)
        state = state + product(hidden, down_ref[...])
        predicted = precise(state, out_ref[...])
        now = jnp.full((8, 128), levels_ref[step].astype(jnp.float32))
        following = levels_ref[jnp.minimum(step + 1, STEPS - 1)]
        after = plan(jnp.full((8, 128), following.astype(jnp.float32)))
        last = jnp.full((8, 128), step) == STEPS - 1
        after = jnp.where(last, 1.0, after)[0:1, 0:10]
        current = plan(now)[0:1, 0:10]
        clean = (sample - jnp.sqrt(1.0 - current) * predicted) / jnp.sqrt(current)
        actions_ref[...] = jnp.sqrt(after) * clean + jnp.sqrt(1.0 - after) * predicted
        return carry

    lax.fori_loop(0, STEPS, one_step, 0)


def denoise(levels, noise, condition, *params):
    whole = pl.BlockSpec(memory_space=VMEM)
    return pl.pallas_call(
        denoise_kernel,
        out_shape=jax.ShapeDtypeStruct((128, 10), jnp.float32),
        in_specs=[pl.BlockSpec(memory_space=pltpu.SMEM)] + [whole] * (2 + len(params)),
        out_specs=whole,
        scratch_shapes=[
            VMEM((8 * KEYS, 1024), jnp.bfloat16),
            VMEM((8, 512), jnp.float32),
            VMEM((128, 1536), jnp.bfloat16),
            VMEM((128, 512), jnp.bfloat16),
        ],
        compiler_params=pltpu.CompilerParams(vmem_limit_bytes=60 * 1024 * 1024),
    )(levels, noise, condition, *params)


def on_device(
    pixels,
    patch_weight,
    position,
    encoder_gains,
    qkv_weight,
    out_weight,
    up_weight,
    down_weight,
    cond_weight,
    time_weight,
    action_in,
    action_pos,
    denoise_gains,
    self_qkv,
    self_out,
    cross_query,
    cross_kv,
    cross_out,
    mix_up,
    mix_down,
    action_out,
    noise,
    timesteps,
):
    local_views, group_count, block_count, patches, pixel_width = pixels.shape
    count = local_views * group_count * block_count
    width = position.shape[1]
    head_size = width // HEADS
    flat = pixels.reshape(count * patches, pixel_width)
    patch_full, qkv_full, out_full, up_full, down_full = (
        lax.all_gather(patch_weight, "mp", axis=0, tiled=True),
        *in_one_piece((qkv_weight, out_weight, up_weight), "mp", 0, 1),
        lax.all_gather(down_weight, "mp", axis=0, tiled=True),
    )
    embedded = product(flat, patch_full)
    state = embedded.reshape(count, patches, width) + position.astype(jnp.float32)
    normed = normalize(state, encoder_gains[0]).astype(jnp.bfloat16).reshape(-1, width)
    packed = (
        product(normed, qkv_full).astype(jnp.bfloat16).reshape(count, patches, 3, HEADS, head_size)
    )
    scores = contract("nqhd,nkhd->nhqk", packed[:, :, 0], packed[:, :, 1]) / math.sqrt(head_size)
    probs = jax.nn.softmax(scores, -1).astype(jnp.bfloat16)
    context = contract("nhqk,nkhd->nqhd", probs, packed[:, :, 2]).astype(jnp.bfloat16)
    state = state + product(context.reshape(-1, width), out_full).reshape(state.shape)
    normed = normalize(state, encoder_gains[1]).astype(jnp.bfloat16).reshape(-1, width)
    hidden = jax.nn.gelu(product(normed, up_full), approximate=False).astype(jnp.bfloat16)
    state = state + product(hidden, down_full).reshape(state.shape)
    side = GRID // 2
    final = normalize(state, encoder_gains[2]).reshape(count, side, 2, side, 2, width)
    cells = side * side
    pooled = jnp.mean(final, axis=(2, 4)).reshape(count, cells, width).astype(jnp.bfloat16)
    condition = product(pooled.reshape(-1, width), cond_weight).astype(jnp.bfloat16)
    condition = jnp.pad(condition.reshape(count, cells, -1), ((0, 0), (0, KEYS - cells), (0, 0)))
    moved = lax.all_to_all(condition, "batch", split_axis=0, concat_axis=0, tiled=True)
    actions = denoise(
        timesteps,
        noise.reshape(-1, noise.shape[-1]),
        moved.reshape(count * KEYS, -1),
        time_weight,
        action_in,
        action_pos,
        denoise_gains,
        self_qkv,
        self_out,
        cross_query,
        cross_kv,
        cross_out,
        mix_up,
        mix_down,
        action_out,
    )
    return actions.reshape(noise.shape)


def solution(mesh):
    return jax.shard_map(
        on_device,
        mesh=mesh,
        in_specs=(
            P("batch", "mp", None, None, None),
            P("mp", None),
            P(),
            P(),
            P("mp", None),
            P("mp", None),
            P("mp", None),
            P("mp", None),
            P(),
            P(),
            P(),
            P(),
            P(),
            P(),
            P(),
            P(),
            P(),
            P(),
            P(),
            P(),
            P(),
            P("mp", "batch", None, None, None),
            P(),
        ),
        out_specs=P("mp", "batch", None, None, None),
        check_vma=False,
    )
```

```python
import math

import jax
import jax.numpy as jnp
from jax import lax
from jax.experimental import pallas as pl
from jax.experimental.pallas import tpu as pltpu
from jax.sharding import PartitionSpec as P

GRID = 10
STEPS = 4
TMAX = 100


norm_eps = 1e-06
offset = 0.008


def normalize(values, gain):
    middle = jnp.mean(values, -1, keepdims=True)
    centred = values - middle
    spread = jnp.mean(centred * centred, -1, keepdims=True)
    return centred * lax.rsqrt(spread + norm_eps) * gain


def plan(level):
    angle = (level.astype(jnp.float32) / TMAX + offset) / (1.0 + offset) * (math.pi / 2)
    base = math.cos(offset / (1.0 + offset) * math.pi / 2) ** 2
    return jnp.cos(angle) ** 2 / base


def product(left, right):
    return jnp.dot(left, right, preferred_element_type=jnp.float32)


def precise(left, right):
    return jnp.dot(left, right, precision=lax.Precision.HIGHEST)


VMEM = pltpu.VMEM
KEYS = 32


def stacked_heads(block):
    lane = lax.broadcasted_iota(jnp.int32, block.shape, 1)
    low = jnp.where(lane < 64, block, jnp.zeros_like(block))
    high = jnp.where(lane < 64, jnp.zeros_like(block), block)
    return jnp.concatenate([low, high], axis=0)


def pair_attention(query, keys, values, allowed):
    rows = query.shape[0]
    scores = lax.dot_general(
        stacked_heads(query), keys, (((1,), (1,)), ((), ())), preferred_element_type=jnp.float32
    )
    scores = jnp.where(allowed, scores * 0.125, -1e30)
    top = jnp.max(scores, axis=-1, keepdims=True)
    grown = jnp.exp(scores - top)
    probs = (grown / jnp.sum(grown, axis=-1, keepdims=True)).astype(jnp.bfloat16)
    both = jnp.dot(probs, values, preferred_element_type=jnp.float32)
    lane = lax.broadcasted_iota(jnp.int32, (rows, 128), 1)
    return jnp.where(lane < 64, both[:rows], both[rows:]).astype(jnp.bfloat16)


def gelu(values):
    return 0.5 * values * (1.0 + lax.erf(values * math.sqrt(0.5)))


def denoise_kernel(
    levels_ref,
    noise_ref,
    condition_ref,
    time_ref,
    in_ref,
    pos_ref,
    gains_ref,
    qkv_ref,
    self_out_ref,
    query_ref,
    kv_ref,
    cross_out_ref,
    up_ref,
    down_ref,
    out_ref,
    actions_ref,
    memory,
    stamps,
    packed,
    context,
):
    width = 512
    rows = 128
    memory[...] = product(condition_ref[...], kv_ref[...]).astype(jnp.bfloat16)
    row = lax.broadcasted_iota(jnp.int32, (8, width // 2), 0)
    level = jnp.zeros((8, width // 2), jnp.float32)
    for step in range(STEPS):
        level = jnp.where(row == step, levels_ref[step].astype(jnp.float32), level)
    order = lax.broadcasted_iota(jnp.int32, (8, width // 2), 1).astype(jnp.float32)
    phase = level * jnp.exp(order * (-math.log(10000.0) / (width // 2)))
    waves = jnp.concatenate([jnp.sin(phase), jnp.cos(phase)], axis=1)
    stamps[...] = precise(waves, time_ref[...])
    actions_ref[...] = noise_ref[...]

    own = lax.broadcasted_iota(jnp.int32, (2 * rows, rows), 0)
    other = lax.broadcasted_iota(jnp.int32, (2 * rows, rows), 1)
    same = lax.rem(own, rows) // 16 == other // 16
    slot = lax.broadcasted_iota(jnp.int32, (2 * rows, 8 * KEYS), 1)
    held = lax.rem(slot, KEYS) < 25

    def one_step(step, carry):
        sample = actions_ref[...]
        state = precise(sample, in_ref[...])
        state = (state.reshape(8, 16, width) + pos_ref[...]).reshape(rows, width)
        state = state + stamps[pl.ds(step, 1), :]
        normed = normalize(state, gains_ref[0:1, :]).astype(jnp.bfloat16)
        packed[...] = product(normed, qkv_ref[...]).astype(jnp.bfloat16)
        for pair in range(4):
            at = pair * 128
            context[:, at : at + 128] = pair_attention(
                packed[:, at : at + 128],
                packed[:, width + at : width + at + 128],
                packed[:, 2 * width + at : 2 * width + at + 128],
                same,
            )
        state = state + product(context[...], self_out_ref[...])
        normed = normalize(state, gains_ref[1:2, :]).astype(jnp.bfloat16)
        packed[:, 0:width] = product(normed, query_ref[...]).astype(jnp.bfloat16)
        for pair in range(4):
            at = pair * 128
            context[:, at : at + 128] = pair_attention(
                packed[:, at : at + 128],
                memory[:, at : at + 128],
                memory[:, width + at : width + at + 128],
                held,
            )
        state = state + product(context[...], cross_out_ref[...])
        normed = normalize(state, gains_ref[2:3, :]).astype(jnp.bfloat16)
        hidden = gelu(product(normed, up_ref[...])).astype(jnp.bfloat16)
        state = state + product(hidden, down_ref[...])
        predicted = precise(state, out_ref[...])
        now = jnp.full((8, 128), levels_ref[step].astype(jnp.float32))
        following = levels_ref[jnp.minimum(step + 1, STEPS - 1)]
        after = plan(jnp.full((8, 128), following.astype(jnp.float32)))
        last = jnp.full((8, 128), step) == STEPS - 1
        after = jnp.where(last, 1.0, after)[0:1, 0:10]
        current = plan(now)[0:1, 0:10]
        clean = (sample - jnp.sqrt(1.0 - current) * predicted) / jnp.sqrt(current)
        actions_ref[...] = jnp.sqrt(after) * clean + jnp.sqrt(1.0 - after) * predicted
        return carry

    lax.fori_loop(0, STEPS, one_step, 0)


def denoise(levels, noise, condition, *params):
    whole = pl.BlockSpec(memory_space=VMEM)
    return pl.pallas_call(
        denoise_kernel,
        out_shape=jax.ShapeDtypeStruct((128, 10), jnp.float32),
        in_specs=[pl.BlockSpec(memory_space=pltpu.SMEM)] + [whole] * (2 + len(params)),
        out_specs=whole,
        scratch_shapes=[
            VMEM((8 * KEYS, 1024), jnp.bfloat16),
            VMEM((8, 512), jnp.float32),
            VMEM((128, 1536), jnp.bfloat16),
            VMEM((128, 512), jnp.bfloat16),
        ],
        compiler_params=pltpu.CompilerParams(vmem_limit_bytes=60 * 1024 * 1024),
    )(levels, noise, condition, *params)


FRAMES = 8
ROWS = 112
LINKS = 24
CHUNKS = 8
MESH = pl.DeviceIdType.MESH


def encode_kernel(
    pixels_ref,
    patch_ref,
    position_ref,
    gains_ref,
    qkv_ref,
    out_ref,
    up_ref,
    down_ref,
    cond_ref,
    result_ref,
    patch_full,
    qkv_full,
    out_full,
    up_full,
    down_full,
    pixels,
    place,
    state,
    normed,
    packed,
    hidden,
    pooled,
    leaving,
    landed,
    sent,
    came,
    kept,
    slab_sent,
    slab_came,
):
    batch = lax.axis_index("batch")
    part = lax.axis_index("mp")
    near, y = batch // 4, batch % 4
    core = part % 2
    z = (part // 2) % 4
    half = part // 8
    kind = (y + near + half) % 2

    def at_z(by):
        return {"mp": (half * 4 + (z + by) % 4) * 2 + core, "batch": batch}

    def at_y(by):
        return {"batch": near * 4 + (y + by) % 4, "mp": part}

    z_up, z_down, y_up, y_down = at_z(1), at_z(3), at_y(1), at_y(3)
    inner = {"batch": (1 - near) * 4 + y, "mp": part}
    cross = {"batch": (1 - near) * 4 + y, "mp": ((1 - half) * 4 + z) * 2 + core}
    partner = {"batch": batch, "mp": part + 1 - 2 * core}

    chunks = (
        (patch_ref, patch_full, 48, 0, 1024),
        (qkv_ref, qkv_full, 64, 0, 1536),
        (qkv_ref, qkv_full, 64, 1536, 1536),
        (out_ref, out_full, 64, 0, 1024),
        (up_ref, up_full, 64, 0, 2048),
        (up_ref, up_full, 64, 2048, 2048),
        (down_ref, down_full, 256, 0, 512),
        (down_ref, down_full, 256, 512, 512),
    )

    def span(chunk, side, which):
        start, width = chunk[3], chunk[4]
        if which == "all":
            return pl.ds(start, width)
        if which == "half":
            return pl.ds(pl.multiple_of(start + side * (width // 2), 128), width // 2)
        first = start + side * (width // 2) + which * (width // 4)
        return pl.ds(pl.multiple_of(first, 128), width // 4)

    def region(chunk, where, holder, side, which):
        other, by = where
        side_half = 1 - half if other else half
        owner = (side_half * 4 + (z + by) % 4) * 2 + holder
        base = pl.multiple_of(owner * chunk[2], 16)
        return chunk[1].at[pl.ds(base, chunk[2]), span(chunk, side, which)]

    own, below, above, far = (0, 0), (0, 3), (0, 1), (0, 2)
    x_own, x_below, x_above, x_far = (1, 0), (1, 3), (1, 1), (1, 2)
    outgoing = (
        (own, "half", z_up),
        (own, "half", z_down),
        (own, "half", cross),
        (below, 0, z_up),
        (above, 1, z_down),
        (x_own, "half", z_up),
        (x_own, "half", z_down),
        (far, "half", cross),
        (below, "half", y_up),
        (x_below, "half", y_up),
        (x_far, 0, y_up),
        (above, "half", y_down),
        (x_above, "half", y_down),
        (x_far, 1, y_down),
        (x_own, "half", inner),
        (far, "half", inner),
        (own, "all", partner),
        (below, "all", partner),
        (above, "all", partner),
        (x_own, "all", partner),
        (x_below, "all", partner),
        (x_above, "all", partner),
        (far, "all", partner),
        (x_far, "all", partner),
    )
    arriving = (
        (below, "half"),
        (above, "half"),
        (x_own, "half"),
        (far, 0),
        (far, 1),
        (x_below, "half"),
        (x_above, "half"),
        (x_far, "half"),
        (below, "half"),
        (x_below, "half"),
        (x_far, 0),
        (above, "half"),
        (x_above, "half"),
        (x_far, 1),
        (x_own, "half"),
        (far, "half"),
        (own, "all"),
        (below, "all"),
        (above, "all"),
        (x_own, "all"),
        (x_below, "all"),
        (x_above, "all"),
        (far, "all"),
        (x_far, "all"),
    )

    def copy_out(k, slot):
        chunk = chunks[k]
        where, which, peer = outgoing[slot]
        target = region(chunk, where, core, kind, which)
        source = chunk[0].at[:, span(chunk, kind, which)] if where == own else target
        return pltpu.make_async_remote_copy(
            src_ref=source,
            dst_ref=target,
            send_sem=sent.at[k, slot],
            recv_sem=came.at[k, slot],
            device_id=peer,
            device_id_type=MESH,
        )

    def keep(k):
        chunk = chunks[k]
        return pltpu.make_async_copy(
            chunk[0].at[:, span(chunk, 0, "all")], region(chunk, own, core, 0, "all"), kept.at[k]
        )

    def send(k, *slots):
        for slot in slots:
            copy_out(k, slot).start()

    def await_slots(k, *slots):
        for slot in slots:
            where, which = arriving[slot]
            holder = core if slot < 16 else 1 - core
            side = kind if slot < 8 else 1 - kind
            place_here = region(chunks[k], where, holder, side, which)
            pltpu.make_async_remote_copy(
                src_ref=place_here,
                dst_ref=place_here,
                send_sem=sent.at[k, slot],
                recv_sem=came.at[k, slot],
                device_id=partner,
                device_id_type=MESH,
            ).wait_recv()

    def s0(k):
        send(k, 0, 1, 2)
        keep(k).start()
        send(k, 16)

    def s1(k):
        await_slots(k, 0, 1, 2)
        send(k, 5, 6, 3, 4, 8, 11, 14)

    def s2(k):
        await_slots(k, 3, 4, 5, 6)
        send(k, 7, 9, 12, 15)

    def s3(k):
        await_slots(k, 8, 11, 14)
        send(k, 17, 18, 19)

    def s4(k):
        await_slots(k, 7)
        send(k, 10, 13)

    def s5(k):
        await_slots(k, 9, 12, 15)
        send(k, 20, 21, 22)

    def s6(k):
        await_slots(k, 10, 13)
        send(k, 23)

    def s7(k):
        keep(k).wait()
        await_slots(k, 16, 17, 18, 19, 20, 21, 22, 23)

    barrier = pltpu.get_barrier_semaphore()
    for peer in (z_up, z_down, cross, partner):
        pl.semaphore_signal(barrier, inc=1, device_id=peer, device_id_type=MESH)
    for by in range(1, FRAMES):
        peer = {"batch": (batch + by) % FRAMES, "mp": part}
        pl.semaphore_signal(barrier, inc=1, device_id=peer, device_id_type=MESH)
    pl.semaphore_wait(barrier, 4 + FRAMES - 1)

    def run(count, body, steps):
        def turn(i, carry):
            for when, act in steps:
                pl.when(i == when)(act)
            body(i)
            return carry

        lax.fori_loop(0, count, turn, 0)

    def norm_rows(gain):
        def one(i):
            rows = pl.ds(pl.multiple_of(i * ROWS, 16), ROWS)
            normed[rows, :] = normalize(state[rows, :], gains_ref[gain : gain + 1, :]).astype(
                jnp.bfloat16
            )

        return one

    def columns(i, width):
        return pl.ds(pl.multiple_of(i * width, 128), width)

    s0(0)
    s0(1)
    for frame in range(FRAMES):
        pixels[frame * ROWS + 96 : (frame + 1) * ROWS, :] = jnp.zeros((16, 768), jnp.bfloat16)
        pixels[frame * ROWS : frame * ROWS + 100, :] = pixels_ref[frame]
    place[96:ROWS, :] = jnp.zeros((16, 1024), jnp.float32)
    place[0:100, :] = position_ref[...].astype(jnp.float32)
    s1(0)
    s0(2)
    s2(0)
    s3(0)
    s1(1)
    s0(3)
    s4(0)
    s5(0)
    s2(1)
    s3(1)
    s6(0)
    s7(0)

    def embed(i):
        cols = columns(i, 512)
        raw = product(pixels[...], patch_full[:, cols]).reshape(FRAMES, ROWS, 512)
        state[:, cols] = (raw + place[:, cols]).reshape(FRAMES * ROWS, 512)

    run(2, embed, ())
    s1(2)
    s0(4)
    s4(1)
    s5(1)
    run(FRAMES, norm_rows(0), ())
    s2(2)
    s3(2)
    s6(1)
    s7(1)

    def pack(start):
        def one(i):
            cols = columns(start + i, 512)
            packed[:, cols] = product(normed[...], qkv_full[:, cols]).astype(jnp.bfloat16)

        return one

    def rest():
        s1(3)
        s0(5)
        s4(2)
        s5(2)
        s6(2)
        s7(2)

    run(6, pack(0), ((3, rest),))

    key_at = lax.broadcasted_iota(jnp.int32, (2 * ROWS, ROWS), 1)

    def attend(frame):
        rows = pl.ds(pl.multiple_of(frame * ROWS, 16), ROWS)
        for pair in range(8):
            at = pair * 128
            normed[rows, at : at + 128] = pair_attention(
                packed[rows, at : at + 128],
                packed[rows, 1024 + at : 1152 + at],
                packed[rows, 2048 + at : 2176 + at],
                key_at < 100,
            )

    def steps(*acts):
        def act():
            for stage, k in acts:
                stage(k)

        return act

    run(
        FRAMES,
        attend,
        (
            (0, steps((s2, 3), (s3, 3), (s1, 4), (s0, 6))),
            (2, steps((s4, 3), (s5, 3), (s2, 4), (s3, 4))),
            (3, steps((s6, 3), (s1, 5), (s0, 7))),
            (4, steps((s4, 4), (s5, 4))),
            (5, steps((s2, 5), (s3, 5), (s6, 4))),
            (6, steps((s1, 6), (s4, 5), (s5, 5))),
            (7, steps((s2, 6), (s3, 6), (s6, 5))),
        ),
    )
    s7(3)

    def project(i):
        cols = columns(i, 512)
        state[:, cols] += product(normed[...], out_full[:, cols])

    run(2, project, ())
    s1(7)
    s4(6)
    s5(6)
    run(FRAMES, norm_rows(1), ())
    s2(7)
    s3(7)
    s6(6)
    s7(4)

    def grow(i):
        cols = columns(i, 512)
        hidden[:, cols] = gelu(product(normed[...], up_full[:, cols])).astype(jnp.bfloat16)

    run(8, grow, ((2, steps((s4, 7), (s5, 7))), (3, steps((s6, 7))), (4, steps((s7, 5)))))
    s7(6)

    def shrink(i):
        cols = columns(i, 512)
        state[:, cols] += product(hidden[...], down_full[:, cols])

    run(2, shrink, ((1, steps((s7, 7))),))

    cell = lax.broadcasted_iota(jnp.int32, (KEYS, ROWS), 0)
    patch = lax.broadcasted_iota(jnp.int32, (KEYS, ROWS), 1)
    home = patch // GRID // 2 * (GRID // 2) + patch % GRID // 2
    share = jnp.where((home == cell) & (patch < 100), 0.25, 0.0).astype(jnp.bfloat16)

    def pool(frame):
        rows = pl.ds(pl.multiple_of(frame * ROWS, 16), ROWS)
        final = normalize(state[rows, :], gains_ref[2:3, :])
        high = final.astype(jnp.bfloat16)
        low = (final - high.astype(jnp.float32)).astype(jnp.bfloat16)
        mean = product(share, high) + product(share, low)
        pooled[pl.ds(pl.multiple_of(frame * KEYS, 16), KEYS), :] = mean.astype(jnp.bfloat16)

    run(FRAMES, pool, ())
    leaving[...] = (
        product(pooled[...], cond_ref[...]).astype(jnp.bfloat16).reshape(FRAMES, KEYS, 512)
    )

    def slab(by):
        to = (batch + by) % FRAMES
        return pltpu.make_async_remote_copy(
            src_ref=leaving.at[to],
            dst_ref=landed.at[batch],
            send_sem=slab_sent.at[by],
            recv_sem=slab_came.at[by],
            device_id={"batch": to, "mp": part},
            device_id_type=MESH,
        )

    for by in range(1, FRAMES):
        slab(by).start()
    for by in range(1, FRAMES):
        source = (batch + FRAMES - by) % FRAMES
        pltpu.make_async_remote_copy(
            src_ref=landed.at[source],
            dst_ref=landed.at[source],
            send_sem=slab_sent.at[by],
            recv_sem=slab_came.at[by],
            device_id=partner,
            device_id_type=MESH,
        ).wait_recv()
        result_ref[source] = landed[source]
    result_ref[batch] = leaving[batch]
    for by in range(1, FRAMES):
        slab(by).wait_send()
    for k in range(CHUNKS):
        for slot in range(LINKS):
            copy_out(k, slot).wait_send()


def encode(pixels, patch, position, gains, qkv, out, up, down, cond):
    bf16, f32 = jnp.bfloat16, jnp.float32
    whole = pl.BlockSpec(memory_space=VMEM)
    apart = pl.BlockSpec(memory_space=pl.ANY)
    tall = FRAMES * ROWS
    return pl.pallas_call(
        encode_kernel,
        out_shape=jax.ShapeDtypeStruct((FRAMES, KEYS, 512), bf16),
        in_specs=[whole, apart, whole, whole, apart, apart, apart, apart, whole],
        out_specs=whole,
        scratch_shapes=[
            VMEM((768, 1024), bf16),
            VMEM((1024, 3072), bf16),
            VMEM((1024, 1024), bf16),
            VMEM((1024, 4096), bf16),
            VMEM((4096, 1024), bf16),
            VMEM((tall, 768), bf16),
            VMEM((ROWS, 1024), f32),
            VMEM((tall, 1024), f32),
            VMEM((tall, 1024), bf16),
            VMEM((tall, 3072), bf16),
            VMEM((tall, 4096), bf16),
            VMEM((FRAMES * KEYS, 1024), bf16),
            VMEM((FRAMES, KEYS, 512), bf16),
            VMEM((FRAMES, KEYS, 512), bf16),
            pltpu.SemaphoreType.DMA((CHUNKS, LINKS)),
            pltpu.SemaphoreType.DMA((CHUNKS, LINKS)),
            pltpu.SemaphoreType.DMA((CHUNKS,)),
            pltpu.SemaphoreType.DMA((FRAMES,)),
            pltpu.SemaphoreType.DMA((FRAMES,)),
        ],
        compiler_params=pltpu.CompilerParams(
            vmem_limit_bytes=67043328, collective_id=0, has_side_effects=True
        ),
    )(pixels, patch, position, gains, qkv, out, up, down, cond)


def on_device(
    pixels,
    patch_weight,
    position,
    encoder_gains,
    qkv_weight,
    out_weight,
    up_weight,
    down_weight,
    cond_weight,
    time_weight,
    action_in,
    action_pos,
    denoise_gains,
    self_qkv,
    self_out,
    cross_query,
    cross_kv,
    cross_out,
    mix_up,
    mix_down,
    action_out,
    noise,
    timesteps,
):
    condition = encode(
        pixels.reshape(pixels.shape[2:]),
        patch_weight,
        position,
        encoder_gains,
        qkv_weight,
        out_weight,
        up_weight,
        down_weight,
        cond_weight,
    )
    actions = denoise(
        timesteps,
        noise.reshape(-1, noise.shape[-1]),
        condition.reshape(FRAMES * KEYS, -1),
        time_weight,
        action_in,
        action_pos,
        denoise_gains,
        self_qkv,
        self_out,
        cross_query,
        cross_kv,
        cross_out,
        mix_up,
        mix_down,
        action_out,
    )
    return actions.reshape(noise.shape)


def solution(mesh):
    return jax.shard_map(
        on_device,
        mesh=mesh,
        in_specs=(
            P("batch", "mp", None, None, None),
            P("mp", None),
            P(),
            P(),
            P("mp", None),
            P("mp", None),
            P("mp", None),
            P("mp", None),
            P(),
            P(),
            P(),
            P(),
            P(),
            P(),
            P(),
            P(),
            P(),
            P(),
            P(),
            P(),
            P(),
            P("mp", "batch", None, None, None),
            P(),
        ),
        out_specs=P("mp", "batch", None, None, None),
        check_vma=False,
    )
```

```python
import functools
import math

import jax
import jax.numpy as jnp
from jax import lax
from jax.experimental import pallas as pl
from jax.experimental.pallas import tpu as pltpu
from jax.sharding import PartitionSpec as P

GRID = 10
STEPS = 4
TMAX = 100


norm_eps = 1e-06
offset = 0.008


def normalize(values, gain):
    middle = jnp.mean(values, -1, keepdims=True)
    centred = values - middle
    spread = jnp.mean(centred * centred, -1, keepdims=True)
    return centred * lax.rsqrt(spread + norm_eps) * gain


def plan(level):
    angle = (level.astype(jnp.float32) / TMAX + offset) / (1.0 + offset) * (math.pi / 2)
    base = math.cos(offset / (1.0 + offset) * math.pi / 2) ** 2
    return jnp.cos(angle) ** 2 / base


def product(left, right):
    return jnp.dot(left, right, preferred_element_type=jnp.float32)


def precise(left, right):
    return jnp.dot(left, right, precision=lax.Precision.HIGHEST)


VMEM = pltpu.VMEM
KEYS = 32


def stacked_heads(block):
    lane = lax.broadcasted_iota(jnp.int32, block.shape, 1)
    low = jnp.where(lane < 64, block, jnp.zeros_like(block))
    high = jnp.where(lane < 64, jnp.zeros_like(block), block)
    return jnp.concatenate([low, high], axis=0)


def pair_attention(query, keys, values, allowed):
    rows = query.shape[0]
    scores = lax.dot_general(
        stacked_heads(query), keys, (((1,), (1,)), ((), ())), preferred_element_type=jnp.float32
    )
    scores = jnp.where(allowed, scores * 0.125, -1e30)
    top = jnp.max(scores, axis=-1, keepdims=True)
    grown = jnp.exp(scores - top)
    probs = (grown / jnp.sum(grown, axis=-1, keepdims=True)).astype(jnp.bfloat16)
    both = jnp.dot(probs, values, preferred_element_type=jnp.float32)
    lane = lax.broadcasted_iota(jnp.int32, (rows, 128), 1)
    return jnp.where(lane < 64, both[:rows], both[rows:]).astype(jnp.bfloat16)


def gelu(values):
    return 0.5 * values * (1.0 + lax.erf(values * math.sqrt(0.5)))


def denoise_kernel(
    levels_ref,
    noise_ref,
    condition_ref,
    time_ref,
    in_ref,
    pos_ref,
    gains_ref,
    qkv_ref,
    self_out_ref,
    query_ref,
    kv_ref,
    cross_out_ref,
    up_ref,
    down_ref,
    out_ref,
    actions_ref,
    memory,
    stamps,
    packed,
    context,
    flat,
    sample_now,
    widened_in,
    widened_out,
):
    width = 512
    rows = 128
    memory[...] = product(condition_ref[...], kv_ref[...]).astype(jnp.bfloat16)
    row = lax.broadcasted_iota(jnp.int32, (8, width // 2), 0)
    level = jnp.zeros((8, width // 2), jnp.float32)
    for step in range(STEPS):
        level = jnp.where(row == step, levels_ref[step].astype(jnp.float32), level)
    order = lax.broadcasted_iota(jnp.int32, (8, width // 2), 1).astype(jnp.float32)
    phase = level * jnp.exp(order * (-math.log(10000.0) / (width // 2)))
    waves = jnp.concatenate([jnp.sin(phase), jnp.cos(phase)], axis=1)
    stamps[...] = precise(waves, time_ref[...])
    for widened, given in ((widened_in, in_ref), (widened_out, out_ref)):
        widened[8:16, :] = jnp.zeros((8, width), jnp.float32)
        widened[0:10, :] = given[...]
    flat[...] = jnp.zeros_like(flat)
    for cand in range(8):
        flat[0:10, cand * 16 : cand * 16 + 16] = noise_ref[:, cand, :]
    sample_now[...] = flat[...].T

    own = lax.broadcasted_iota(jnp.int32, (2 * rows, rows), 0)
    other = lax.broadcasted_iota(jnp.int32, (2 * rows, rows), 1)
    same = lax.rem(own, rows) // 16 == other // 16
    slot = lax.broadcasted_iota(jnp.int32, (2 * rows, 8 * KEYS), 1)
    held = lax.rem(slot, KEYS) < 25

    def one_step(step, carry):
        sample = sample_now[...]
        state = precise(sample, widened_in[...])
        state = (state.reshape(8, 16, width) + pos_ref[...]).reshape(rows, width)
        state = state + stamps[pl.ds(step, 1), :]
        normed = normalize(state, gains_ref[0:1, :]).astype(jnp.bfloat16)
        packed[...] = product(normed, qkv_ref[...]).astype(jnp.bfloat16)
        for pair in range(4):
            at = pair * 128
            context[:, at : at + 128] = pair_attention(
                packed[:, at : at + 128],
                packed[:, width + at : width + at + 128],
                packed[:, 2 * width + at : 2 * width + at + 128],
                same,
            )
        state = state + product(context[...], self_out_ref[...])
        normed = normalize(state, gains_ref[1:2, :]).astype(jnp.bfloat16)
        packed[:, 0:width] = product(normed, query_ref[...]).astype(jnp.bfloat16)
        for pair in range(4):
            at = pair * 128
            context[:, at : at + 128] = pair_attention(
                packed[:, at : at + 128],
                memory[:, at : at + 128],
                memory[:, width + at : width + at + 128],
                held,
            )
        state = state + product(context[...], cross_out_ref[...])
        normed = normalize(state, gains_ref[2:3, :]).astype(jnp.bfloat16)
        hidden = gelu(product(normed, up_ref[...])).astype(jnp.bfloat16)
        state = state + product(hidden, down_ref[...])
        predicted = lax.dot_general(
            state,
            widened_out[...],
            (((1,), (1,)), ((), ())),
            precision=lax.Precision.HIGHEST,
            preferred_element_type=jnp.float32,
        )
        now = jnp.full((8, 128), levels_ref[step].astype(jnp.float32))
        following = levels_ref[jnp.minimum(step + 1, STEPS - 1)]
        after = plan(jnp.full((8, 128), following.astype(jnp.float32)))
        last = jnp.full((8, 128), step) == STEPS - 1
        after = jnp.where(last, 1.0, after)[0:1, 0:16]
        current = plan(now)[0:1, 0:16]
        clean = (sample - jnp.sqrt(1.0 - current) * predicted) / jnp.sqrt(current)
        sample_now[...] = jnp.sqrt(after) * clean + jnp.sqrt(1.0 - after) * predicted
        return carry

    lax.fori_loop(0, STEPS, one_step, 0)
    flat[...] = sample_now[...].T
    for cand in range(8):
        actions_ref[:, cand, :] = flat[0:10, cand * 16 : cand * 16 + 16]


def denoise(levels, noise, condition, *params):
    whole = pl.BlockSpec(memory_space=VMEM)
    return pl.pallas_call(
        denoise_kernel,
        out_shape=jax.ShapeDtypeStruct((10, 8, 16), jnp.float32),
        in_specs=[pl.BlockSpec(memory_space=pltpu.SMEM)] + [whole] * (2 + len(params)),
        out_specs=whole,
        scratch_shapes=[
            VMEM((8 * KEYS, 1024), jnp.bfloat16),
            VMEM((8, 512), jnp.float32),
            VMEM((128, 1536), jnp.bfloat16),
            VMEM((128, 512), jnp.bfloat16),
            VMEM((16, 128), jnp.float32),
            VMEM((128, 16), jnp.float32),
            VMEM((16, 512), jnp.float32),
            VMEM((16, 512), jnp.float32),
        ],
        compiler_params=pltpu.CompilerParams(vmem_limit_bytes=60 * 1024 * 1024),
    )(levels, noise, condition, *params)


FRAMES = 8
ROWS = 112
LINKS = 24
CHUNKS = 8
MESH = pl.DeviceIdType.MESH
PLAN = {
    "prepare": (
        (0, "a0", "a1", "a2", "b0", "o4", "c0", "b1", "c1", "d0", "o2", "b2", "o5", "a3",),
    ),
    "embed": (
        (0, "c2", "e0", "d1", "f1", "g0", "e1", "f0", "o0", "a4", "o1", "d2", "c3", "h0", "i0", "g1", "f2", "a5", "b3", "a6", "a7", "o7", "z0",),
        (1, "e2", "h1",),
    ),
    "first_norm": (
        (0, "i1",),
        (1, "o3",),
        (5, "g2",),
    ),
    "qkv": (
        (0, "z1",),
        (1, "h2", "c4",),
        (2, "b4", "i2", "e3",),
        (3, "d3", "f3", "b5", "c5", "z2",),
    ),
    "att": (
        (0, "f4", "b6",),
        (2, "h3", "g3", "c6", "b7",),
        (3, "d4", "f5", "e4",),
        (4, "d5", "c7",),
        (6, "g4",),
        (7, "e5", "i3", "d6",),
    ),
    "out": (
        (0, "o6", "z3", "e6", "h4",),
        (1, "g5",),
    ),
    "second_norm": (
        (2, "i4",),
        (3, "d7", "h5", "f6", "e7",),
        (4, "g6",),
    ),
    "up": (
        (0, "z4",),
        (2, "i5",),
        (3, "h6", "g7",),
        (4, "z5",),
        (6, "i6",),
        (7, "h7",),
    ),
    "down": (
        (0, "f7", "i7", "z6",),
        (1, "z7",),
    ),
    "tail": (
    ),
}


def encode_kernel(
    pixels_ref,
    patch_ref,
    position_ref,
    gains_ref,
    qkv_ref,
    out_ref,
    up_ref,
    down_ref,
    cond_ref,
    result_ref,
    patch_full,
    qkv_full,
    out_full,
    up_full,
    down_full,
    spread,
    pixels,
    place,
    state,
    normed,
    packed,
    hidden,
    pooled,
    leaving,
    landed,
    sent,
    came,
    kept,
    slab_sent,
    slab_came,
):
    batch = lax.axis_index("batch")
    part = lax.axis_index("mp")
    near, y = batch // 4, batch % 4
    core = part % 2
    z = (part // 2) % 4
    half = part // 8
    kind = (y + near + half) % 2

    def at_z(by):
        return {"mp": (half * 4 + (z + by) % 4) * 2 + core, "batch": batch}

    def at_y(by):
        return {"batch": near * 4 + (y + by) % 4, "mp": part}

    z_up, z_down, y_up, y_down = at_z(1), at_z(3), at_y(1), at_y(3)
    inner = {"batch": (1 - near) * 4 + y, "mp": part}
    cross = {"batch": (1 - near) * 4 + y, "mp": ((1 - half) * 4 + z) * 2 + core}
    partner = {"batch": batch, "mp": part + 1 - 2 * core}

    chunks = (
        (patch_ref, patch_full, 48, 0, 1024),
        (qkv_ref, qkv_full, 64, 0, 1536),
        (qkv_ref, qkv_full, 64, 1536, 1536),
        (out_ref, out_full, 64, 0, 1024),
        (up_ref, up_full, 64, 0, 2048),
        (up_ref, up_full, 64, 2048, 2048),
        (down_ref, down_full, 256, 0, 512),
        (down_ref, down_full, 256, 512, 512),
    )

    def span(chunk, side, which):
        start, width = chunk[3], chunk[4]
        if which == "all":
            return pl.ds(start, width)
        if which == "half":
            return pl.ds(pl.multiple_of(start + side * (width // 2), 128), width // 2)
        first = start + side * (width // 2) + which * (width // 4)
        return pl.ds(pl.multiple_of(first, 128), width // 4)

    def region(chunk, where, holder, side, which):
        other, by = where
        side_half = 1 - half if other else half
        owner = (side_half * 4 + (z + by) % 4) * 2 + holder
        base = pl.multiple_of(owner * chunk[2], 16)
        return chunk[1].at[pl.ds(base, chunk[2]), span(chunk, side, which)]

    own, below, above, far = (0, 0), (0, 3), (0, 1), (0, 2)
    x_own, x_below, x_above, x_far = (1, 0), (1, 3), (1, 1), (1, 2)
    outgoing = (
        (own, "half", z_up),
        (own, "half", z_down),
        (own, "half", cross),
        (below, 0, z_up),
        (above, 1, z_down),
        (x_own, "half", z_up),
        (x_own, "half", z_down),
        (far, "half", cross),
        (below, "half", y_up),
        (x_below, "half", y_up),
        (x_far, 0, y_up),
        (above, "half", y_down),
        (x_above, "half", y_down),
        (x_far, 1, y_down),
        (x_own, "half", inner),
        (far, "half", inner),
        (own, "all", partner),
        (below, "all", partner),
        (above, "all", partner),
        (x_own, "all", partner),
        (x_below, "all", partner),
        (x_above, "all", partner),
        (far, "all", partner),
        (x_far, "all", partner),
    )
    arriving = (
        (below, "half"),
        (above, "half"),
        (x_own, "half"),
        (far, 0),
        (far, 1),
        (x_below, "half"),
        (x_above, "half"),
        (x_far, "half"),
        (below, "half"),
        (x_below, "half"),
        (x_far, 0),
        (above, "half"),
        (x_above, "half"),
        (x_far, 1),
        (x_own, "half"),
        (far, "half"),
        (own, "all"),
        (below, "all"),
        (above, "all"),
        (x_own, "all"),
        (x_below, "all"),
        (x_above, "all"),
        (far, "all"),
        (x_far, "all"),
    )

    def copy_out(k, slot):
        chunk = chunks[k]
        where, which, peer = outgoing[slot]
        target = region(chunk, where, core, kind, which)
        source = chunk[0].at[:, span(chunk, kind, which)] if where == own else target
        return pltpu.make_async_remote_copy(
            src_ref=source,
            dst_ref=target,
            send_sem=sent.at[k, slot],
            recv_sem=came.at[k, slot],
            device_id=peer,
            device_id_type=MESH,
        )

    def keep(k):
        chunk = chunks[k]
        return pltpu.make_async_copy(
            chunk[0].at[:, span(chunk, 0, "all")], region(chunk, own, core, 0, "all"), kept.at[k]
        )

    def send(k, *slots):
        for slot in slots:
            copy_out(k, slot).start()

    def await_slots(k, *slots):
        for slot in slots:
            where, which = arriving[slot]
            holder = core if slot < 16 else 1 - core
            side = kind if slot < 8 else 1 - kind
            place_here = region(chunks[k], where, holder, side, which)
            pltpu.make_async_remote_copy(
                src_ref=place_here,
                dst_ref=place_here,
                send_sem=sent.at[k, slot],
                recv_sem=came.at[k, slot],
                device_id=partner,
                device_id_type=MESH,
            ).wait_recv()

    moves = {
        "a": ((), (0, 1, 2)),
        "o": ((), (16,)),
        "b": ((0, 1), (3, 4, 8, 11)),
        "c": ((2,), (5, 6, 14)),
        "d": ((3, 4), (7, 15)),
        "e": ((5, 6), (9, 12)),
        "f": ((8, 11, 14), (17, 18, 19)),
        "g": ((7,), (10, 13)),
        "h": ((9, 12, 15), (20, 21, 22)),
        "i": ((10, 13), (23,)),
        "z": ((16, 17, 18, 19, 20, 21, 22, 23), ()),
    }

    def move(names):
        for name in names:
            k = int(name[1])
            awaited, sending = moves[name[0]]
            if name[0] == "o":
                keep(k).start()
            if name[0] == "z":
                keep(k).wait()
            await_slots(k, *awaited)
            send(k, *sending)

    barrier = pltpu.get_barrier_semaphore()
    for peer in (z_up, z_down, cross, partner):
        pl.semaphore_signal(barrier, inc=1, device_id=peer, device_id_type=MESH)
    for by in range(1, FRAMES):
        peer = {"batch": (batch + by) % FRAMES, "mp": part}
        pl.semaphore_signal(barrier, inc=1, device_id=peer, device_id_type=MESH)
    pl.semaphore_wait(barrier, 4 + FRAMES - 1)

    def run(count, body, stage):
        def turn(i, carry):
            for when, *names in PLAN.get(stage, ()):
                pl.when(i == when)(functools.partial(move, names))
            body(i)
            return carry

        lax.fori_loop(0, count, turn, 0)

    def norm_rows(gain):
        def one(i):
            rows = pl.ds(pl.multiple_of(i * ROWS, 16), ROWS)
            normed[rows, :] = normalize(state[rows, :], gains_ref[gain : gain + 1, :]).astype(
                jnp.bfloat16
            )

        return one

    def columns(i, width):
        return pl.ds(pl.multiple_of(i * width, 128), width)

    move(PLAN["prepare"][0][1:])
    for part_at in range(6):
        lanes = pl.ds(part_at * 128, 128)
        spread[part_at] = pixels_ref[:, :, lanes].astype(jnp.float32).reshape(800, 128)
    for frame in range(FRAMES):
        pixels[frame * ROWS + 96 : (frame + 1) * ROWS, :] = jnp.zeros((16, 768), jnp.bfloat16)
        for part_at in range(6):
            pixels[frame * ROWS : frame * ROWS + 100, part_at * 128 : part_at * 128 + 128] = spread[
                part_at, pl.ds(frame, 100, stride=FRAMES), :
            ].astype(jnp.bfloat16)
    place[96:ROWS, :] = jnp.zeros((16, 1024), jnp.float32)
    place[0:100, :] = position_ref[...].astype(jnp.float32)

    def embed(i):
        cols = columns(i, 512)
        raw = product(pixels[...], patch_full[:, cols]).reshape(FRAMES, ROWS, 512)
        state[:, cols] = (raw + place[:, cols]).reshape(FRAMES * ROWS, 512)

    run(2, embed, "embed")
    run(FRAMES, norm_rows(0), "first_norm")

    def pack(i):
        cols = columns(i, 512)
        packed[:, cols] = product(normed[...], qkv_full[:, cols]).astype(jnp.bfloat16)

    run(6, pack, "qkv")

    key_at = lax.broadcasted_iota(jnp.int32, (2 * ROWS, ROWS), 1)

    def attend(frame):
        rows = pl.ds(pl.multiple_of(frame * ROWS, 16), ROWS)
        for pair in range(8):
            at = pair * 128
            normed[rows, at : at + 128] = pair_attention(
                packed[rows, at : at + 128],
                packed[rows, 1024 + at : 1152 + at],
                packed[rows, 2048 + at : 2176 + at],
                key_at < 100,
            )

    run(FRAMES, attend, "att")

    def project(i):
        cols = columns(i, 512)
        state[:, cols] += product(normed[...], out_full[:, cols])

    run(2, project, "out")
    run(FRAMES, norm_rows(1), "second_norm")

    def grow(i):
        cols = columns(i, 512)
        hidden[:, cols] = gelu(product(normed[...], up_full[:, cols])).astype(jnp.bfloat16)

    run(8, grow, "up")

    def shrink(i):
        cols = columns(i, 512)
        state[:, cols] += product(hidden[...], down_full[:, cols])

    run(2, shrink, "down")

    cell = lax.broadcasted_iota(jnp.int32, (KEYS, ROWS), 0)
    patch = lax.broadcasted_iota(jnp.int32, (KEYS, ROWS), 1)
    home = patch // GRID // 2 * (GRID // 2) + patch % GRID // 2
    share = jnp.where((home == cell) & (patch < 100), 0.25, 0.0).astype(jnp.bfloat16)

    def pool(frame):
        rows = pl.ds(pl.multiple_of(frame * ROWS, 16), ROWS)
        final = normalize(state[rows, :], gains_ref[2:3, :])
        high = final.astype(jnp.bfloat16)
        low = (final - high.astype(jnp.float32)).astype(jnp.bfloat16)
        mean = product(share, high) + product(share, low)
        pooled[pl.ds(pl.multiple_of(frame * KEYS, 16), KEYS), :] = mean.astype(jnp.bfloat16)

    run(FRAMES, pool, "tail")
    leaving[...] = (
        product(pooled[...], cond_ref[...]).astype(jnp.bfloat16).reshape(FRAMES, KEYS, 512)
    )

    def slab(by):
        to = (batch + by) % FRAMES
        return pltpu.make_async_remote_copy(
            src_ref=leaving.at[to],
            dst_ref=landed.at[batch],
            send_sem=slab_sent.at[by],
            recv_sem=slab_came.at[by],
            device_id={"batch": to, "mp": part},
            device_id_type=MESH,
        )

    for by in range(1, FRAMES):
        slab(by).start()
    for by in range(1, FRAMES):
        source = (batch + FRAMES - by) % FRAMES
        pltpu.make_async_remote_copy(
            src_ref=landed.at[source],
            dst_ref=landed.at[source],
            send_sem=slab_sent.at[by],
            recv_sem=slab_came.at[by],
            device_id=partner,
            device_id_type=MESH,
        ).wait_recv()
        result_ref[source] = landed[source]
    result_ref[batch] = leaving[batch]
    for by in range(1, FRAMES):
        slab(by).wait_send()
    for k in range(CHUNKS):
        for slot in range(LINKS):
            copy_out(k, slot).wait_send()


def encode(pixels, patch, position, gains, qkv, out, up, down, cond):
    bf16, f32 = jnp.bfloat16, jnp.float32
    whole = pl.BlockSpec(memory_space=VMEM)
    apart = pl.BlockSpec(memory_space=pl.ANY)
    tall = FRAMES * ROWS
    return pl.pallas_call(
        encode_kernel,
        out_shape=jax.ShapeDtypeStruct((FRAMES, KEYS, 512), bf16),
        in_specs=[whole, apart, whole, whole, apart, apart, apart, apart, whole],
        out_specs=whole,
        scratch_shapes=[
            VMEM((768, 1024), bf16),
            VMEM((1024, 3072), bf16),
            VMEM((1024, 1024), bf16),
            VMEM((1024, 4096), bf16),
            VMEM((4096, 1024), bf16),
            VMEM((6, 800, 128), f32),
            VMEM((tall, 768), bf16),
            VMEM((ROWS, 1024), f32),
            VMEM((tall, 1024), f32),
            VMEM((tall, 1024), bf16),
            VMEM((tall, 3072), bf16),
            VMEM((tall, 4096), bf16),
            VMEM((FRAMES * KEYS, 1024), bf16),
            VMEM((FRAMES, KEYS, 512), bf16),
            VMEM((FRAMES, KEYS, 512), bf16),
            pltpu.SemaphoreType.DMA((CHUNKS, LINKS)),
            pltpu.SemaphoreType.DMA((CHUNKS, LINKS)),
            pltpu.SemaphoreType.DMA((CHUNKS,)),
            pltpu.SemaphoreType.DMA((FRAMES,)),
            pltpu.SemaphoreType.DMA((FRAMES,)),
        ],
        compiler_params=pltpu.CompilerParams(
            vmem_limit_bytes=67043328, collective_id=0, has_side_effects=True
        ),
    )(pixels, patch, position, gains, qkv, out, up, down, cond)


def on_device(
    pixels,
    patch_weight,
    position,
    encoder_gains,
    qkv_weight,
    out_weight,
    up_weight,
    down_weight,
    cond_weight,
    time_weight,
    action_in,
    action_pos,
    denoise_gains,
    self_qkv,
    self_out,
    cross_query,
    cross_kv,
    cross_out,
    mix_up,
    mix_down,
    action_out,
    noise,
    timesteps,
):
    condition = encode(
        jnp.transpose(pixels.reshape(pixels.shape[2:]), (1, 0, 2)),
        patch_weight,
        position,
        encoder_gains,
        qkv_weight,
        out_weight,
        up_weight,
        down_weight,
        cond_weight,
    )
    actions = denoise(
        timesteps,
        jnp.transpose(noise.reshape(noise.shape[2:]), (2, 0, 1)),
        condition.reshape(FRAMES * KEYS, -1),
        time_weight,
        action_in,
        action_pos,
        denoise_gains,
        self_qkv,
        self_out,
        cross_query,
        cross_kv,
        cross_out,
        mix_up,
        mix_down,
        action_out.T,
    )
    return jnp.transpose(actions, (1, 2, 0)).reshape(noise.shape)


def solution(mesh):
    return jax.shard_map(
        on_device,
        mesh=mesh,
        in_specs=(
            P("batch", "mp", None, None, None),
            P("mp", None),
            P(),
            P(),
            P("mp", None),
            P("mp", None),
            P("mp", None),
            P("mp", None),
            P(),
            P(),
            P(),
            P(),
            P(),
            P(),
            P(),
            P(),
            P(),
            P(),
            P(),
            P(),
            P(),
            P("mp", "batch", None, None, None),
            P(),
        ),
        out_specs=P("mp", "batch", None, None, None),
        check_vma=False,
    )
```

```python
import functools
import math

import jax
import jax.numpy as jnp
from jax import lax
from jax.experimental import pallas as pl
from jax.experimental.pallas import tpu as pltpu
from jax.sharding import PartitionSpec as P

GRID = 10
STEPS = 4
TMAX = 100


norm_eps = 1e-06
offset = 0.008


def normalize(values, gain):
    middle = jnp.mean(values, -1, keepdims=True)
    centred = values - middle
    spread = jnp.mean(centred * centred, -1, keepdims=True)
    return centred * lax.rsqrt(spread + norm_eps) * gain


def plan(level):
    angle = (level.astype(jnp.float32) / TMAX + offset) / (1.0 + offset) * (math.pi / 2)
    base = math.cos(offset / (1.0 + offset) * math.pi / 2) ** 2
    return jnp.cos(angle) ** 2 / base


def product(left, right):
    return jnp.dot(left, right, preferred_element_type=jnp.float32)


def precise(left, right):
    return jnp.dot(left, right, precision=lax.Precision.HIGHEST)


VMEM = pltpu.VMEM
KEYS = 32


def stacked_heads(block):
    lane = lax.broadcasted_iota(jnp.int32, block.shape, 1)
    low = jnp.where(lane < 64, block, jnp.zeros_like(block))
    high = jnp.where(lane < 64, jnp.zeros_like(block), block)
    return jnp.concatenate([low, high], axis=0)


def pair_attention(query, keys, values, allowed):
    rows = query.shape[0]
    scores = lax.dot_general(
        stacked_heads(query), keys, (((1,), (1,)), ((), ())), preferred_element_type=jnp.float32
    )
    scores = jnp.where(allowed, scores * (0.125 * math.log2(math.e)), -1e30)
    top = jnp.max(scores, axis=-1, keepdims=True)
    grown = jnp.exp2(scores - top)
    inverse = 1.0 / jnp.sum(grown, axis=-1, keepdims=True)
    probs = (grown * inverse).astype(jnp.bfloat16)
    both = jnp.dot(probs, values, preferred_element_type=jnp.float32)
    lane = lax.broadcasted_iota(jnp.int32, (rows, 128), 1)
    return jnp.where(lane < 64, both[:rows], both[rows:]).astype(jnp.bfloat16)


def gelu(values):
    return 0.5 * values * (1.0 + lax.erf(values * math.sqrt(0.5)))


def denoiser(
    levels_ref,
    condition,
    noise_ref,
    time_ref,
    in_ref,
    pos_ref,
    gains_ref,
    qkv_ref,
    self_out_ref,
    query_ref,
    kv_ref,
    cross_out_ref,
    up_ref,
    down_ref,
    out_ref,
    actions_ref,
    memory,
    stamps,
    packed,
    context,
    flat,
    sample_now,
    widened_in,
    widened_out,
    out_columns,
    held_state,
):
    width = 512
    rows = 128

    def first_half(step):
        own = lax.broadcasted_iota(jnp.int32, (2 * rows, rows), 0)
        other = lax.broadcasted_iota(jnp.int32, (2 * rows, rows), 1)
        same = lax.rem(own, rows) // 16 == other // 16
        state = precise(sample_now[...], widened_in[...])
        state = (state.reshape(8, 16, width) + pos_ref[...]).reshape(rows, width)
        state = state + stamps[pl.ds(step, 1), :]
        normed = normalize(state, gains_ref[0:1, :]).astype(jnp.bfloat16)
        packed[...] = product(normed, qkv_ref[...]).astype(jnp.bfloat16)
        for pair in range(4):
            at = pair * 128
            context[:, at : at + 128] = pair_attention(
                packed[:, at : at + 128],
                packed[:, width + at : width + at + 128],
                packed[:, 2 * width + at : 2 * width + at + 128],
                same,
            )
        held_state[...] = state + product(context[...], self_out_ref[...])

    def begin():
        row = lax.broadcasted_iota(jnp.int32, (8, width // 2), 0)
        level = jnp.zeros((8, width // 2), jnp.float32)
        for step in range(STEPS):
            level = jnp.where(row == step, levels_ref[step].astype(jnp.float32), level)
        order = lax.broadcasted_iota(jnp.int32, (8, width // 2), 1).astype(jnp.float32)
        phase = level * jnp.exp(order * (-math.log(10000.0) / (width // 2)))
        waves = jnp.concatenate([jnp.sin(phase), jnp.cos(phase)], axis=1)
        stamps[...] = precise(waves, time_ref[...])
        for widened, given in ((widened_in, in_ref), (widened_out, out_ref)):
            widened[8:16, :] = jnp.zeros((8, width), jnp.float32)
            widened[0:10, :] = given[...]
        out_columns[...] = widened_out[...].T
        flat[...] = jnp.zeros_like(flat)
        for cand in range(8):
            flat[0:10, cand * 16 : cand * 16 + 16] = noise_ref[:, cand, :]
        sample_now[...] = flat[...].T
        first_half(0)

    def one_step(step, carry):
        slot = lax.broadcasted_iota(jnp.int32, (2 * rows, 8 * KEYS), 1)
        held = lax.rem(slot, KEYS) < 25
        sample = sample_now[...]
        state = held_state[...]
        normed = normalize(state, gains_ref[1:2, :]).astype(jnp.bfloat16)
        packed[:, 0:width] = product(normed, query_ref[...]).astype(jnp.bfloat16)
        for pair in range(4):
            at = pair * 128
            context[:, at : at + 128] = pair_attention(
                packed[:, at : at + 128],
                memory[:, at : at + 128],
                memory[:, width + at : width + at + 128],
                held,
            )
        state = state + product(context[...], cross_out_ref[...])
        normed = normalize(state, gains_ref[2:3, :]).astype(jnp.bfloat16)
        hidden = gelu(product(normed, up_ref[...])).astype(jnp.bfloat16)
        state = state + product(hidden, down_ref[...])
        predicted = precise(state, out_columns[...])
        now = jnp.full((8, 128), levels_ref[step].astype(jnp.float32))
        following = levels_ref[jnp.minimum(step + 1, STEPS - 1)]
        after = plan(jnp.full((8, 128), following.astype(jnp.float32)))
        last = jnp.full((8, 128), step) == STEPS - 1
        after = jnp.where(last, 1.0, after)[0:1, 0:16]
        current = plan(now)[0:1, 0:16]
        clean = (sample - jnp.sqrt(1.0 - current) * predicted) / jnp.sqrt(current)
        sample_now[...] = jnp.sqrt(after) * clean + jnp.sqrt(1.0 - after) * predicted
        pl.when(step < STEPS - 1)(lambda: first_half(step + 1))
        return carry

    def finish():
        memory[...] = product(condition[...].reshape(8 * KEYS, width), kv_ref[...]).astype(
            jnp.bfloat16
        )
        lax.fori_loop(0, STEPS, one_step, 0)
        flat[...] = sample_now[...].T
        for cand in range(8):
            actions_ref[:, cand, :] = flat[0:10, cand * 16 : cand * 16 + 16]

    return begin, finish


FRAMES = 8
ROWS = 112
LINKS = 24
CHUNKS = 8
MESH = pl.DeviceIdType.MESH
PLAN = {
    "prepare": (
        ("a0", "a1", "o0", "a2", "o1",),
        ("b0", "c0", "b1", "c1", "o5", "a3", "o7", "d0", "b2", "e0", "c2", "d1", "g0", "a4", "f0", "f1", "o2", "o3", "c3", "e1",),
        ("h0", "g1", "d2", "i0", "e2", "a5", "b3", "f2", "h1", "z0",),
    ),
    "embed": (
    ),
    "first_norm": (
        (0, "i1",),
        (2, "c4",),
        (3, "g2",),
        (6, "b4",),
        (7, "z1", "h2",),
    ),
    "qkv": (
        (0, "a6", "o4",),
        (2, "i2", "f3", "e3", "d3", "b5",),
        (3, "c5", "z2",),
        (4, "e4",),
        (5, "d4", "a7", "f4",),
    ),
    "att": (
        (0, "g3",),
        (2, "h3", "d5",),
        (3, "b6",),
        (4, "i3", "g4", "f5", "h4", "c6",),
        (5, "e5",),
        (7, "d6", "b7", "z3", "c7", "i4", "g5",),
    ),
    "out": (
    ),
    "second_norm": (
        (1, "d7", "e6", "z4",),
        (4, "h5", "g6",),
    ),
    "up": (
        (1, "e7", "i5", "f6", "o6",),
        (3, "z5", "h6", "g7",),
        (6, "i6", "f7",),
    ),
    "down": (
        (0, "z6", "h7", "i7",),
        (1, "z7",),
    ),
    "tail": (
    ),
}


DENOISER = (
    ((10, 8, 16), jnp.float32),
    ((512, 512), jnp.float32),
    ((10, 512), jnp.float32),
    ((16, 512), jnp.float32),
    ((3, 512), jnp.float32),
    ((512, 1536), jnp.bfloat16),
    ((512, 512), jnp.bfloat16),
    ((512, 512), jnp.bfloat16),
    ((512, 1024), jnp.bfloat16),
    ((512, 512), jnp.bfloat16),
    ((512, 2048), jnp.bfloat16),
    ((2048, 512), jnp.bfloat16),
    ((10, 512), jnp.float32),
)
BROUGHT = len(DENOISER) + 4


def whole_kernel(*refs):
    levels_ref = refs[0]
    given = refs[1 : 10 + len(DENOISER)]
    actions_ref = refs[10 + len(DENOISER)]
    rest = refs[11 + len(DENOISER) :]
    encode_kernel(levels_ref, given, actions_ref, rest[:BROUGHT], rest[BROUGHT : BROUGHT + 10], *rest[BROUGHT + 10 :])


def encode_kernel(
    levels_ref,
    given,
    actions_ref,
    held,
    denoiser_scratch,
    patch_full,
    qkv_full,
    out_full,
    up_full,
    down_full,
    spread,
    place,
    state,
    normed,
    packed,
    hidden,
    pooled,
    leaving,
    landed,
    sent,
    came,
    kept,
    slab_sent,
    slab_came,
    brought,
):
    pixels_in, patch_ref, position_in, gains_in, qkv_ref, out_ref, up_ref, down_ref, cond_in = given[:9]
    pixels_ref, position_ref, gains_ref, cond_ref = held[:4]
    pixels = hidden.at[:, 0:768]
    incoming = (pixels_in, position_in, gains_in, cond_in, *given[9:])

    def bring(i):
        return pltpu.make_async_copy(incoming[i], held[i], brought.at[i])

    begin, finish = denoiser(
        levels_ref, landed, *held[4:], actions_ref, *denoiser_scratch
    )
    batch = lax.axis_index("batch")
    part = lax.axis_index("mp")
    near, y = batch // 4, batch % 4
    core = part % 2
    z = (part // 2) % 4
    half = part // 8
    kind = (y + near + half) % 2

    def at_z(by):
        return {"mp": (half * 4 + (z + by) % 4) * 2 + core, "batch": batch}

    def at_y(by):
        return {"batch": near * 4 + (y + by) % 4, "mp": part}

    z_up, z_down, y_up, y_down = at_z(1), at_z(3), at_y(1), at_y(3)
    inner = {"batch": (1 - near) * 4 + y, "mp": part}
    cross = {"batch": (1 - near) * 4 + y, "mp": ((1 - half) * 4 + z) * 2 + core}
    partner = {"batch": batch, "mp": part + 1 - 2 * core}

    chunks = (
        (patch_ref, patch_full, 48, 0, 1024),
        (qkv_ref, qkv_full, 64, 0, 1536),
        (qkv_ref, qkv_full, 64, 1536, 1536),
        (out_ref, out_full, 64, 0, 1024),
        (up_ref, up_full, 64, 0, 2048),
        (up_ref, up_full, 64, 2048, 2048),
        (down_ref, down_full, 256, 0, 512),
        (down_ref, down_full, 256, 512, 512),
    )

    def span(chunk, side, which):
        start, width = chunk[3], chunk[4]
        if which == "all":
            return pl.ds(start, width)
        if which == "half":
            return pl.ds(pl.multiple_of(start + side * (width // 2), 128), width // 2)
        first = start + side * (width // 2) + which * (width // 4)
        return pl.ds(pl.multiple_of(first, 128), width // 4)

    def region(chunk, where, holder, side, which):
        other, by = where
        side_half = 1 - half if other else half
        owner = (side_half * 4 + (z + by) % 4) * 2 + holder
        base = pl.multiple_of(owner * chunk[2], 16)
        return chunk[1].at[pl.ds(base, chunk[2]), span(chunk, side, which)]

    own, below, above, far = (0, 0), (0, 3), (0, 1), (0, 2)
    x_own, x_below, x_above, x_far = (1, 0), (1, 3), (1, 1), (1, 2)
    outgoing = (
        (own, "half", z_up),
        (own, "half", z_down),
        (own, "half", cross),
        (below, 0, z_up),
        (above, 1, z_down),
        (x_own, "half", z_up),
        (x_own, "half", z_down),
        (far, "half", cross),
        (below, "half", y_up),
        (x_below, "half", y_up),
        (x_far, 0, y_up),
        (above, "half", y_down),
        (x_above, "half", y_down),
        (x_far, 1, y_down),
        (x_own, "half", inner),
        (far, "half", inner),
        (own, "all", partner),
        (below, "all", partner),
        (above, "all", partner),
        (x_own, "all", partner),
        (x_below, "all", partner),
        (x_above, "all", partner),
        (far, "all", partner),
        (x_far, "all", partner),
    )
    arriving = (
        (below, "half"),
        (above, "half"),
        (x_own, "half"),
        (far, 0),
        (far, 1),
        (x_below, "half"),
        (x_above, "half"),
        (x_far, "half"),
        (below, "half"),
        (x_below, "half"),
        (x_far, 0),
        (above, "half"),
        (x_above, "half"),
        (x_far, 1),
        (x_own, "half"),
        (far, "half"),
        (own, "all"),
        (below, "all"),
        (above, "all"),
        (x_own, "all"),
        (x_below, "all"),
        (x_above, "all"),
        (far, "all"),
        (x_far, "all"),
    )

    def copy_out(k, slot):
        chunk = chunks[k]
        where, which, peer = outgoing[slot]
        target = region(chunk, where, core, kind, which)
        source = chunk[0].at[:, span(chunk, kind, which)] if where == own else target
        return pltpu.make_async_remote_copy(
            src_ref=source,
            dst_ref=target,
            send_sem=sent.at[k, slot],
            recv_sem=came.at[k, slot],
            device_id=peer,
            device_id_type=MESH,
        )

    def keep(k):
        chunk = chunks[k]
        return pltpu.make_async_copy(
            chunk[0].at[:, span(chunk, 0, "all")], region(chunk, own, core, 0, "all"), kept.at[k]
        )

    def send(k, *slots):
        for slot in slots:
            copy_out(k, slot).start()

    def await_slots(k, *slots):
        for slot in slots:
            where, which = arriving[slot]
            holder = core if slot < 16 else 1 - core
            side = kind if slot < 8 else 1 - kind
            place_here = region(chunks[k], where, holder, side, which)
            pltpu.make_async_remote_copy(
                src_ref=place_here,
                dst_ref=place_here,
                send_sem=sent.at[k, slot],
                recv_sem=came.at[k, slot],
                device_id=partner,
                device_id_type=MESH,
            ).wait_recv()

    moves = {
        "a": ((), (0, 1, 2)),
        "o": ((), (16,)),
        "b": ((0, 1), (3, 4, 8, 11)),
        "c": ((2,), (5, 6, 14)),
        "d": ((3, 4), (7, 15)),
        "e": ((5, 6), (9, 12)),
        "f": ((8, 11, 14), (17, 18, 19)),
        "g": ((7,), (10, 13)),
        "h": ((9, 12, 15), (20, 21, 22)),
        "i": ((10, 13), (23,)),
        "z": ((16, 17, 18, 19, 20, 21, 22, 23), ()),
    }

    def move(names):
        for name in names:
            k = int(name[1])
            awaited, sending = moves[name[0]]
            if name[0] == "o":
                keep(k).start()
            if name[0] == "z":
                keep(k).wait()
            await_slots(k, *awaited)
            send(k, *sending)

    barrier = pltpu.get_barrier_semaphore()
    for peer in (z_up, z_down, cross, partner):
        pl.semaphore_signal(barrier, inc=1, device_id=peer, device_id_type=MESH)
    for by in range(1, FRAMES):
        peer = {"batch": (batch + by) % FRAMES, "mp": part}
        pl.semaphore_signal(barrier, inc=1, device_id=peer, device_id_type=MESH)
    pl.semaphore_wait(barrier, 4 + FRAMES - 1)

    def run(count, body, stage):
        def turn(i, carry):
            for when, *names in PLAN.get(stage, ()):
                pl.when(i == when)(functools.partial(move, names))
            body(i)
            return carry

        lax.fori_loop(0, count, turn, 0)

    def norm_rows(gain):
        def one(i):
            rows = pl.ds(pl.multiple_of(i * ROWS, 16), ROWS)
            normed[rows, :] = normalize(state[rows, :], gains_ref[gain : gain + 1, :]).astype(
                jnp.bfloat16
            )

        return one

    def columns(i, width):
        return pl.ds(pl.multiple_of(i * width, 128), width)

    first, second, third = PLAN["prepare"]
    move(first)
    for i in range(BROUGHT):
        bring(i).start()
    for i in range(BROUGHT):
        bring(i).wait()
    for part_at in range(6):
        lanes = pl.ds(part_at * 128, 128)
        spread[...] = pixels_ref[:, :, lanes].astype(jnp.float32).reshape(800, 128)
        for frame in range(FRAMES):
            if part_at == 0:
                pixels[frame * ROWS + 96 : (frame + 1) * ROWS, :] = jnp.zeros(
                    (16, 768), jnp.bfloat16
                )
            pixels[frame * ROWS : frame * ROWS + 100, part_at * 128 : part_at * 128 + 128] = spread[
                pl.ds(frame, 100, stride=FRAMES), :
            ].astype(jnp.bfloat16)
    place[96:ROWS, :] = jnp.zeros((16, 1024), jnp.float32)
    place[0:100, :] = position_ref[...].astype(jnp.float32)
    move(second)
    begin()
    move(third)

    def embed(i):
        cols = columns(i, 512)
        raw = product(pixels[...], patch_full[:, cols]).reshape(FRAMES, ROWS, 512)
        state[:, cols] = (raw + place[:, cols]).reshape(FRAMES * ROWS, 512)

    run(2, embed, "embed")
    run(FRAMES, norm_rows(0), "first_norm")

    def pack(i):
        cols = columns(i, 512)
        packed[:, cols] = product(normed[...], qkv_full[:, cols]).astype(jnp.bfloat16)

    run(6, pack, "qkv")

    key_at = lax.broadcasted_iota(jnp.int32, (2 * ROWS, ROWS), 1)

    def attend(frame):
        rows = pl.ds(pl.multiple_of(frame * ROWS, 16), ROWS)
        for pair in range(8):
            at = pair * 128
            normed[rows, at : at + 128] = pair_attention(
                packed[rows, at : at + 128],
                packed[rows, 1024 + at : 1152 + at],
                packed[rows, 2048 + at : 2176 + at],
                key_at < 100,
            )

    run(FRAMES, attend, "att")

    def project(i):
        cols = columns(i, 512)
        state[:, cols] += product(normed[...], out_full[:, cols])

    run(2, project, "out")
    run(FRAMES, norm_rows(1), "second_norm")

    def grow(i):
        cols = columns(i, 512)
        hidden[:, cols] = gelu(product(normed[...], up_full[:, cols])).astype(jnp.bfloat16)

    run(8, grow, "up")

    def shrink(i):
        cols = columns(i, 512)
        state[:, cols] += product(hidden[...], down_full[:, cols])

    run(2, shrink, "down")

    cell = lax.broadcasted_iota(jnp.int32, (KEYS, ROWS), 0)
    patch = lax.broadcasted_iota(jnp.int32, (KEYS, ROWS), 1)
    home = patch // GRID // 2 * (GRID // 2) + patch % GRID // 2
    share = jnp.where((home == cell) & (patch < 100), 0.25, 0.0).astype(jnp.bfloat16)

    def pool(frame):
        rows = pl.ds(pl.multiple_of(frame * ROWS, 16), ROWS)
        final = normalize(state[rows, :], gains_ref[2:3, :])
        high = final.astype(jnp.bfloat16)
        low = (final - high.astype(jnp.float32)).astype(jnp.bfloat16)
        mean = product(share, high) + product(share, low)
        pooled[pl.ds(pl.multiple_of(frame * KEYS, 16), KEYS), :] = mean.astype(jnp.bfloat16)

    run(FRAMES, pool, "tail")
    leaving[...] = (
        product(pooled[...], cond_ref[...]).astype(jnp.bfloat16).reshape(FRAMES, KEYS, 512)
    )

    def slab(by):
        to = (batch + by) % FRAMES
        return pltpu.make_async_remote_copy(
            src_ref=leaving.at[to],
            dst_ref=landed.at[batch],
            send_sem=slab_sent.at[by],
            recv_sem=slab_came.at[by],
            device_id={"batch": to, "mp": part},
            device_id_type=MESH,
        )

    for by in range(1, FRAMES):
        slab(by).start()
    for by in range(1, FRAMES):
        source = (batch + FRAMES - by) % FRAMES
        pltpu.make_async_remote_copy(
            src_ref=landed.at[source],
            dst_ref=landed.at[source],
            send_sem=slab_sent.at[by],
            recv_sem=slab_came.at[by],
            device_id=partner,
            device_id_type=MESH,
        ).wait_recv()
    landed[batch] = leaving[batch]
    finish()
    for by in range(1, FRAMES):
        slab(by).wait_send()
    for k in range(CHUNKS):
        for slot in range(LINKS):
            copy_out(k, slot).wait_send()


def run_all(levels, *arrays):
    bf16, f32 = jnp.bfloat16, jnp.float32
    apart = pl.BlockSpec(memory_space=pl.ANY)
    tall = FRAMES * ROWS
    return pl.pallas_call(
        whole_kernel,
        out_shape=jax.ShapeDtypeStruct((10, 8, 16), f32),
        in_specs=[pl.BlockSpec(memory_space=pltpu.SMEM)] + [apart] * len(arrays),
        out_specs=pl.BlockSpec(memory_space=VMEM),
        scratch_shapes=[
            VMEM((100, FRAMES, 768), bf16),
            VMEM((100, 1024), bf16),
            VMEM((3, 1024), f32),
            VMEM((1024, 512), bf16),
            *[VMEM(shape, kind) for shape, kind in DENOISER],
            VMEM((8 * KEYS, 1024), bf16),
            VMEM((8, 512), f32),
            VMEM((128, 1536), bf16),
            VMEM((128, 512), bf16),
            VMEM((16, 128), f32),
            VMEM((128, 16), f32),
            VMEM((16, 512), f32),
            VMEM((16, 512), f32),
            VMEM((512, 16), f32),
            VMEM((128, 512), f32),
            VMEM((768, 1024), bf16),
            VMEM((1024, 3072), bf16),
            VMEM((1024, 1024), bf16),
            VMEM((1024, 4096), bf16),
            VMEM((4096, 1024), bf16),
            VMEM((800, 128), f32),
            VMEM((ROWS, 1024), f32),
            VMEM((tall, 1024), f32),
            VMEM((tall, 1024), bf16),
            VMEM((tall, 3072), bf16),
            VMEM((tall, 4096), bf16),
            VMEM((FRAMES * KEYS, 1024), bf16),
            VMEM((FRAMES, KEYS, 512), bf16),
            VMEM((FRAMES, KEYS, 512), bf16),
            pltpu.SemaphoreType.DMA((CHUNKS, LINKS)),
            pltpu.SemaphoreType.DMA((CHUNKS, LINKS)),
            pltpu.SemaphoreType.DMA((CHUNKS,)),
            pltpu.SemaphoreType.DMA((FRAMES,)),
            pltpu.SemaphoreType.DMA((FRAMES,)),
            pltpu.SemaphoreType.DMA((BROUGHT,)),
        ],
        compiler_params=pltpu.CompilerParams(
            vmem_limit_bytes=67043328, collective_id=0, has_side_effects=True
        ),
    )(levels, *arrays)


def on_device(
    pixels,
    patch_weight,
    position,
    encoder_gains,
    qkv_weight,
    out_weight,
    up_weight,
    down_weight,
    cond_weight,
    time_weight,
    action_in,
    action_pos,
    denoise_gains,
    self_qkv,
    self_out,
    cross_query,
    cross_kv,
    cross_out,
    mix_up,
    mix_down,
    action_out,
    noise,
    timesteps,
):
    actions = run_all(
        timesteps,
        jnp.transpose(pixels.reshape(pixels.shape[2:]), (1, 0, 2)),
        patch_weight,
        position,
        encoder_gains,
        qkv_weight,
        out_weight,
        up_weight,
        down_weight,
        cond_weight,
        jnp.transpose(noise.reshape(noise.shape[2:]), (2, 0, 1)),
        time_weight,
        action_in,
        action_pos,
        denoise_gains,
        self_qkv,
        self_out,
        cross_query,
        cross_kv,
        cross_out,
        mix_up,
        mix_down,
        action_out.T,
    )
    return jnp.transpose(actions, (1, 2, 0)).reshape(noise.shape)


def solution(mesh):
    return jax.shard_map(
        on_device,
        mesh=mesh,
        in_specs=(
            P("batch", "mp", None, None, None),
            P("mp", None),
            P(),
            P(),
            P("mp", None),
            P("mp", None),
            P("mp", None),
            P("mp", None),
            P(),
            P(),
            P(),
            P(),
            P(),
            P(),
            P(),
            P(),
            P(),
            P(),
            P(),
            P(),
            P(),
            P("mp", "batch", None, None, None),
            P(),
        ),
        out_specs=P("mp", "batch", None, None, None),
        check_vma=False,
    )
```

```python
import functools
import math

import jax
import jax.numpy as jnp
from jax import lax
from jax.experimental import pallas as pl
from jax.experimental.pallas import tpu as pltpu
from jax.sharding import PartitionSpec as P

GRID = 10
STEPS = 4
TMAX = 100


norm_eps = 1e-06
offset = 0.008


def normalize(values, gain):
    middle = jnp.mean(values, -1, keepdims=True)
    centred = values - middle
    spread = jnp.mean(centred * centred, -1, keepdims=True)
    return centred * lax.rsqrt(spread + norm_eps) * gain


def plan(level):
    angle = (level.astype(jnp.float32) / TMAX + offset) / (1.0 + offset) * (math.pi / 2)
    base = math.cos(offset / (1.0 + offset) * math.pi / 2) ** 2
    return jnp.cos(angle) ** 2 / base


def product(left, right):
    return jnp.dot(left, right, preferred_element_type=jnp.float32)


def precise(left, right):
    return jnp.dot(left, right, precision=lax.Precision.HIGHEST)


VMEM = pltpu.VMEM
KEYS = 32


def stacked_heads(block):
    lane = lax.broadcasted_iota(jnp.int32, block.shape, 1)
    low = jnp.where(lane < 64, block, jnp.zeros_like(block))
    high = jnp.where(lane < 64, jnp.zeros_like(block), block)
    return jnp.concatenate([low, high], axis=0)


def pair_attention(query, keys, values, allowed):
    rows = query.shape[0]
    scores = lax.dot_general(
        stacked_heads(query), keys, (((1,), (1,)), ((), ())), preferred_element_type=jnp.float32
    )
    scores = jnp.where(allowed, scores * (0.125 * math.log2(math.e)), -1e30)
    top = jnp.max(scores, axis=-1, keepdims=True)
    grown = jnp.exp2(scores - top)
    inverse = 1.0 / jnp.sum(grown, axis=-1, keepdims=True)
    probs = (grown * inverse).astype(jnp.bfloat16)
    both = jnp.dot(probs, values, preferred_element_type=jnp.float32)
    lane = lax.broadcasted_iota(jnp.int32, (rows, 128), 1)
    return jnp.where(lane < 64, both[:rows], both[rows:]).astype(jnp.bfloat16)


def gelu(values):
    small = 0.5 * values
    return small + small * lax.erf(values * math.sqrt(0.5))


def denoiser(
    levels_ref,
    condition,
    noise_ref,
    time_ref,
    in_ref,
    pos_ref,
    gains_ref,
    qkv_ref,
    self_out_ref,
    query_ref,
    kv_ref,
    cross_out_ref,
    up_ref,
    down_ref,
    out_ref,
    actions_ref,
    memory,
    stamps,
    packed,
    context,
    flat,
    sample_now,
    widened_in,
    widened_out,
    out_columns,
    held_state,
):
    width = 512
    rows = 128

    def first_half(step):
        own = lax.broadcasted_iota(jnp.int32, (2 * rows, rows), 0)
        other = lax.broadcasted_iota(jnp.int32, (2 * rows, rows), 1)
        same = lax.rem(own, rows) // 16 == other // 16
        state = precise(sample_now[...], widened_in[...])
        state = (state.reshape(8, 16, width) + pos_ref[...]).reshape(rows, width)
        state = state + stamps[pl.ds(step, 1), :]
        normed = normalize(state, gains_ref[0:1, :]).astype(jnp.bfloat16)
        packed[...] = product(normed, qkv_ref[...]).astype(jnp.bfloat16)
        for pair in range(4):
            at = pair * 128
            context[:, at : at + 128] = pair_attention(
                packed[:, at : at + 128],
                packed[:, width + at : width + at + 128],
                packed[:, 2 * width + at : 2 * width + at + 128],
                same,
            )
        state = state + product(context[...], self_out_ref[...])
        held_state[...] = state
        normed = normalize(state, gains_ref[1:2, :]).astype(jnp.bfloat16)
        packed[:, 0:width] = product(normed, query_ref[...]).astype(jnp.bfloat16)

    def begin():
        row = lax.broadcasted_iota(jnp.int32, (8, width // 2), 0)
        level = jnp.zeros((8, width // 2), jnp.float32)
        for step in range(STEPS):
            level = jnp.where(row == step, levels_ref[step].astype(jnp.float32), level)
        order = lax.broadcasted_iota(jnp.int32, (8, width // 2), 1).astype(jnp.float32)
        phase = level * jnp.exp(order * (-math.log(10000.0) / (width // 2)))
        waves = jnp.concatenate([jnp.sin(phase), jnp.cos(phase)], axis=1)
        stamps[...] = precise(waves, time_ref[...])
        for widened, given in ((widened_in, in_ref), (widened_out, out_ref)):
            widened[8:16, :] = jnp.zeros((8, width), jnp.float32)
            widened[0:10, :] = given[...]
        out_columns[...] = widened_out[...].T
        flat[...] = jnp.zeros_like(flat)
        for cand in range(8):
            flat[0:10, cand * 16 : cand * 16 + 16] = noise_ref[:, cand, :]
        sample_now[...] = flat[...].T
        first_half(0)

    def one_step(step, carry):
        slot = lax.broadcasted_iota(jnp.int32, (2 * rows, 8 * KEYS), 1)
        held = lax.rem(slot, KEYS) < 25
        sample = sample_now[...]
        state = held_state[...]
        for pair in range(4):
            at = pair * 128
            context[:, at : at + 128] = pair_attention(
                packed[:, at : at + 128],
                memory[:, at : at + 128],
                memory[:, width + at : width + at + 128],
                held,
            )
        state = state + product(context[...], cross_out_ref[...])
        normed = normalize(state, gains_ref[2:3, :]).astype(jnp.bfloat16)
        hidden = gelu(product(normed, up_ref[...])).astype(jnp.bfloat16)
        state = state + product(hidden, down_ref[...])
        predicted = precise(state, out_columns[...])
        now = jnp.full((8, 128), levels_ref[step].astype(jnp.float32))
        following = levels_ref[jnp.minimum(step + 1, STEPS - 1)]
        after = plan(jnp.full((8, 128), following.astype(jnp.float32)))
        last = jnp.full((8, 128), step) == STEPS - 1
        after = jnp.where(last, 1.0, after)[0:1, 0:16]
        current = plan(now)[0:1, 0:16]
        clean = (sample - jnp.sqrt(1.0 - current) * predicted) / jnp.sqrt(current)
        sample_now[...] = jnp.sqrt(after) * clean + jnp.sqrt(1.0 - after) * predicted
        pl.when(step < STEPS - 1)(lambda: first_half(step + 1))
        return carry

    def finish():
        memory[...] = product(condition[...].reshape(8 * KEYS, width), kv_ref[...]).astype(
            jnp.bfloat16
        )
        lax.fori_loop(0, STEPS, one_step, 0)
        flat[...] = sample_now[...].T
        for cand in range(8):
            actions_ref[:, cand, :] = flat[0:10, cand * 16 : cand * 16 + 16]

    return begin, finish


FRAMES = 8
ROWS = 112
LINKS = 24
CHUNKS = 9
MESH = pl.DeviceIdType.MESH
PLAN = {
    "prepare": (
        ("a0", "a1", "a3", "a2",),
        ("o8", "o6", "b0", "o2", "c0", "o0", "b1", "c1", "a4", "b3", "d0", "b2", "o3", "f0", "c2", "c3", "e0", "a5",),
        ("d1", "g0", "e1", "o1", "d2", "h0", "b4", "e2", "c4", "d3", "i0", "o7", "f1", "g1", "f2", "a6", "z0",),
    ),
    "embed": (
        (1, "g2", "e3",),
    ),
    "first_norm": (
        (0, "h1", "g3",),
        (2, "b5", "d4",),
        (3, "c5", "i1",),
        (6, "e4",),
        (7, "h2", "a7", "i2",),
    ),
    "qkv": (
        (0, "z1", "f3",),
        (1, "g4", "i3", "b6", "h3", "f4", "z2", "d5",),
        (2, "f5", "z3", "o4", "a8", "c6", "o5", "e5",),
    ),
    "att": (
        (1, "h4", "g5",),
        (2, "b7", "c7", "d6",),
        (4, "h5", "i4", "f6", "b8",),
        (6, "c8", "e6",),
        (7, "z4", "d7", "i5", "f7", "g6",),
    ),
    "out": (
        (1, "e7",),
    ),
    "second_norm": (
        (0, "d8",),
        (4, "h6",),
        (5, "z5",),
    ),
    "up": (
        (0, "g7", "e8", "i6",),
        (1, "f8",),
        (2, "g8", "z6", "h7",),
        (3, "i7", "h8",),
    ),
    "down": (
        (0, "z7", "i8",),
        (1, "z8",),
    ),
    "tail": (
    ),
}


DENOISER = (
    ((10, 8, 16), jnp.float32),
    ((512, 512), jnp.float32),
    ((10, 512), jnp.float32),
    ((16, 512), jnp.float32),
    ((3, 512), jnp.float32),
    ((512, 1536), jnp.bfloat16),
    ((512, 512), jnp.bfloat16),
    ((512, 512), jnp.bfloat16),
    ((512, 1024), jnp.bfloat16),
    ((512, 512), jnp.bfloat16),
    ((512, 2048), jnp.bfloat16),
    ((2048, 512), jnp.bfloat16),
    ((10, 512), jnp.float32),
)
BROUGHT = len(DENOISER) + 4


def whole_kernel(*refs):
    levels_ref = refs[0]
    given = refs[1 : 10 + len(DENOISER)]
    actions_ref = refs[10 + len(DENOISER)]
    rest = refs[11 + len(DENOISER) :]
    encode_kernel(levels_ref, given, actions_ref, rest[:BROUGHT], rest[BROUGHT : BROUGHT + 10], *rest[BROUGHT + 10 :])


def encode_kernel(
    levels_ref,
    given,
    actions_ref,
    held,
    denoiser_scratch,
    patch_full,
    qkv_full,
    out_full,
    up_full,
    down_full,
    spread,
    place,
    state,
    normed,
    packed,
    hidden,
    pooled,
    leaving,
    landed,
    sent,
    came,
    kept,
    slab_sent,
    slab_came,
    brought,
):
    pixels_in, patch_ref, position_in, gains_in, qkv_ref, out_ref, up_ref, down_ref, cond_in = given[:9]
    pixels_ref, position_ref, gains_ref, cond_ref = held[:4]
    pixels = hidden.at[:, 0:768]
    incoming = (pixels_in, position_in, gains_in, cond_in, *given[9:])

    def bring(i):
        return pltpu.make_async_copy(incoming[i], held[i], brought.at[i])

    begin, finish = denoiser(
        levels_ref, landed, *held[4:], actions_ref, *denoiser_scratch
    )
    batch = lax.axis_index("batch")
    part = lax.axis_index("mp")
    near, y = batch // 4, batch % 4
    core = part % 2
    z = (part // 2) % 4
    half = part // 8
    kind = (y + near + half) % 2

    def at_z(by):
        return {"mp": (half * 4 + (z + by) % 4) * 2 + core, "batch": batch}

    def at_y(by):
        return {"batch": near * 4 + (y + by) % 4, "mp": part}

    z_up, z_down, y_up, y_down = at_z(1), at_z(3), at_y(1), at_y(3)
    inner = {"batch": (1 - near) * 4 + y, "mp": part}
    cross = {"batch": (1 - near) * 4 + y, "mp": ((1 - half) * 4 + z) * 2 + core}
    partner = {"batch": batch, "mp": part + 1 - 2 * core}

    chunks = (
        (patch_ref, patch_full, 48, 0, 1024),
        (qkv_ref, qkv_full, 64, 0, 1024),
        (qkv_ref, qkv_full, 64, 1024, 1024),
        (qkv_ref, qkv_full, 64, 2048, 1024),
        (out_ref, out_full, 64, 0, 1024),
        (up_ref, up_full, 64, 0, 2048),
        (up_ref, up_full, 64, 2048, 2048),
        (down_ref, down_full, 256, 0, 512),
        (down_ref, down_full, 256, 512, 512),
    )

    def span(chunk, side, which):
        start, width = chunk[3], chunk[4]
        if which == "all":
            return pl.ds(start, width)
        if which == "half":
            return pl.ds(pl.multiple_of(start + side * (width // 2), 128), width // 2)
        first = start + side * (width // 2) + which * (width // 4)
        return pl.ds(pl.multiple_of(first, 128), width // 4)

    def region(chunk, where, holder, side, which):
        other, by = where
        side_half = 1 - half if other else half
        owner = (side_half * 4 + (z + by) % 4) * 2 + holder
        base = pl.multiple_of(owner * chunk[2], 16)
        return chunk[1].at[pl.ds(base, chunk[2]), span(chunk, side, which)]

    own, below, above, far = (0, 0), (0, 3), (0, 1), (0, 2)
    x_own, x_below, x_above, x_far = (1, 0), (1, 3), (1, 1), (1, 2)
    outgoing = (
        (own, "half", z_up),
        (own, "half", z_down),
        (own, "half", cross),
        (below, 0, z_up),
        (above, 1, z_down),
        (x_own, "half", z_up),
        (x_own, "half", z_down),
        (far, "half", cross),
        (below, "half", y_up),
        (x_below, "half", y_up),
        (x_far, 0, y_up),
        (above, "half", y_down),
        (x_above, "half", y_down),
        (x_far, 1, y_down),
        (x_own, "half", inner),
        (far, "half", inner),
        (own, "all", partner),
        (below, "all", partner),
        (above, "all", partner),
        (x_own, "all", partner),
        (x_below, "all", partner),
        (x_above, "all", partner),
        (far, "all", partner),
        (x_far, "all", partner),
    )
    arriving = (
        (below, "half"),
        (above, "half"),
        (x_own, "half"),
        (far, 0),
        (far, 1),
        (x_below, "half"),
        (x_above, "half"),
        (x_far, "half"),
        (below, "half"),
        (x_below, "half"),
        (x_far, 0),
        (above, "half"),
        (x_above, "half"),
        (x_far, 1),
        (x_own, "half"),
        (far, "half"),
        (own, "all"),
        (below, "all"),
        (above, "all"),
        (x_own, "all"),
        (x_below, "all"),
        (x_above, "all"),
        (far, "all"),
        (x_far, "all"),
    )

    def copy_out(k, slot):
        chunk = chunks[k]
        where, which, peer = outgoing[slot]
        target = region(chunk, where, core, kind, which)
        source = chunk[0].at[:, span(chunk, kind, which)] if where == own else target
        return pltpu.make_async_remote_copy(
            src_ref=source,
            dst_ref=target,
            send_sem=sent.at[k, slot],
            recv_sem=came.at[k, slot],
            device_id=peer,
            device_id_type=MESH,
        )

    def keep(k):
        chunk = chunks[k]
        return pltpu.make_async_copy(
            chunk[0].at[:, span(chunk, 0, "all")], region(chunk, own, core, 0, "all"), kept.at[k]
        )

    def send(k, *slots):
        for slot in slots:
            copy_out(k, slot).start()

    def await_slots(k, *slots):
        for slot in slots:
            where, which = arriving[slot]
            holder = core if slot < 16 else 1 - core
            side = kind if slot < 8 else 1 - kind
            place_here = region(chunks[k], where, holder, side, which)
            pltpu.make_async_remote_copy(
                src_ref=place_here,
                dst_ref=place_here,
                send_sem=sent.at[k, slot],
                recv_sem=came.at[k, slot],
                device_id=partner,
                device_id_type=MESH,
            ).wait_recv()

    moves = {
        "a": ((), (0, 1, 2)),
        "o": ((), (16,)),
        "b": ((0, 1), (3, 4, 8, 11)),
        "c": ((2,), (5, 6, 14)),
        "d": ((3, 4), (7, 15)),
        "e": ((5, 6), (9, 12)),
        "f": ((8, 11, 14), (17, 18, 19)),
        "g": ((7,), (10, 13)),
        "h": ((9, 12, 15), (20, 21, 22)),
        "i": ((10, 13), (23,)),
        "z": ((16, 17, 18, 19, 20, 21, 22, 23), ()),
    }

    def move(names):
        for name in names:
            k = int(name[1])
            awaited, sending = moves[name[0]]
            if name[0] == "o":
                keep(k).start()
            if name[0] == "z":
                keep(k).wait()
            await_slots(k, *awaited)
            send(k, *sending)

    barrier = pltpu.get_barrier_semaphore()
    for peer in (z_up, z_down, cross, partner):
        pl.semaphore_signal(barrier, inc=1, device_id=peer, device_id_type=MESH)
    for by in range(1, FRAMES):
        peer = {"batch": (batch + by) % FRAMES, "mp": part}
        pl.semaphore_signal(barrier, inc=1, device_id=peer, device_id_type=MESH)
    pl.semaphore_wait(barrier, 4 + FRAMES - 1)

    def run(count, body, stage):
        def turn(i, carry):
            for when, *names in PLAN.get(stage, ()):
                pl.when(i == when)(functools.partial(move, names))
            body(i)
            return carry

        lax.fori_loop(0, count, turn, 0)

    def norm_rows(gain):
        def one(i):
            rows = pl.ds(pl.multiple_of(i * ROWS, 16), ROWS)
            normed[rows, :] = normalize(state[rows, :], gains_ref[gain : gain + 1, :]).astype(
                jnp.bfloat16
            )

        return one

    def columns(i, width):
        return pl.ds(pl.multiple_of(i * width, 128), width)

    first, second, third = PLAN["prepare"]
    move(first)
    for i in range(BROUGHT):
        bring(i).start()
    for i in range(BROUGHT):
        bring(i).wait()
    for part_at in range(6):
        lanes = pl.ds(part_at * 128, 128)
        spread[...] = pixels_ref[:, :, lanes].astype(jnp.float32).reshape(800, 128)
        for frame in range(FRAMES):
            if part_at == 0:
                pixels[frame * ROWS + 96 : (frame + 1) * ROWS, :] = jnp.zeros(
                    (16, 768), jnp.bfloat16
                )
            pixels[frame * ROWS : frame * ROWS + 100, part_at * 128 : part_at * 128 + 128] = spread[
                pl.ds(frame, 100, stride=FRAMES), :
            ].astype(jnp.bfloat16)
    place[96:ROWS, :] = jnp.zeros((16, 1024), jnp.float32)
    place[0:100, :] = position_ref[...].astype(jnp.float32)
    move(second)
    begin()
    move(third)

    def embed(i):
        cols = columns(i, 512)
        raw = product(pixels[...], patch_full[:, cols]).reshape(FRAMES, ROWS, 512)
        state[:, cols] = (raw + place[:, cols]).reshape(FRAMES * ROWS, 512)

    run(2, embed, "embed")
    run(FRAMES, norm_rows(0), "first_norm")

    def pack(i):
        cols = columns(i, 1024)
        packed[:, cols] = product(normed[...], qkv_full[:, cols]).astype(jnp.bfloat16)

    run(3, pack, "qkv")

    key_at = lax.broadcasted_iota(jnp.int32, (2 * ROWS, ROWS), 1)

    def attend(frame):
        rows = pl.ds(pl.multiple_of(frame * ROWS, 16), ROWS)
        for pair in range(8):
            at = pair * 128
            normed[rows, at : at + 128] = pair_attention(
                packed[rows, at : at + 128],
                packed[rows, 1024 + at : 1152 + at],
                packed[rows, 2048 + at : 2176 + at],
                key_at < 100,
            )

    run(FRAMES, attend, "att")

    def project(i):
        rows = pl.ds(pl.multiple_of(i * 448, 16), 448)
        grown = state[rows, :] + product(normed[rows, :], out_full[...])
        state[rows, :] = grown
        normed[rows, :] = normalize(grown, gains_ref[1:2, :]).astype(jnp.bfloat16)

    run(2, project, "out")
    for _, *names in PLAN["second_norm"]:
        move(names)

    def grow(i):
        cols = columns(i, 1024)
        hidden[:, cols] = gelu(product(normed[...], up_full[:, cols])).astype(jnp.bfloat16)

    run(4, grow, "up")

    def shrink(i):
        cols = columns(i, 512)
        state[:, cols] += product(hidden[...], down_full[:, cols])

    run(2, shrink, "down")

    cell = lax.broadcasted_iota(jnp.int32, (KEYS, ROWS), 0)
    patch = lax.broadcasted_iota(jnp.int32, (KEYS, ROWS), 1)
    home = patch // GRID // 2 * (GRID // 2) + patch % GRID // 2
    share = jnp.where((home == cell) & (patch < 100), 0.25, 0.0).astype(jnp.bfloat16)

    def pool(frame):
        rows = pl.ds(pl.multiple_of(frame * ROWS, 16), ROWS)
        final = normalize(state[rows, :], gains_ref[2:3, :])
        high = final.astype(jnp.bfloat16)
        low = (final - high.astype(jnp.float32)).astype(jnp.bfloat16)
        mean = product(share, high) + product(share, low)
        pooled[pl.ds(pl.multiple_of(frame * KEYS, 16), KEYS), :] = mean.astype(jnp.bfloat16)

    run(FRAMES, pool, "tail")
    leaving[...] = (
        product(pooled[...], cond_ref[...]).astype(jnp.bfloat16).reshape(FRAMES, KEYS, 512)
    )

    def slab(by):
        to = (batch + by) % FRAMES
        return pltpu.make_async_remote_copy(
            src_ref=leaving.at[to],
            dst_ref=landed.at[batch],
            send_sem=slab_sent.at[by],
            recv_sem=slab_came.at[by],
            device_id={"batch": to, "mp": part},
            device_id_type=MESH,
        )

    for by in range(1, FRAMES):
        slab(by).start()
    for k in range(CHUNKS):
        for slot in range(LINKS):
            copy_out(k, slot).wait_send()
    landed[batch] = leaving[batch]
    for by in range(1, FRAMES):
        source = (batch + FRAMES - by) % FRAMES
        pltpu.make_async_remote_copy(
            src_ref=landed.at[source],
            dst_ref=landed.at[source],
            send_sem=slab_sent.at[by],
            recv_sem=slab_came.at[by],
            device_id=partner,
            device_id_type=MESH,
        ).wait_recv()
    finish()
    for by in range(1, FRAMES):
        slab(by).wait_send()


def run_all(levels, *arrays):
    bf16, f32 = jnp.bfloat16, jnp.float32
    apart = pl.BlockSpec(memory_space=pl.ANY)
    tall = FRAMES * ROWS
    return pl.pallas_call(
        whole_kernel,
        out_shape=jax.ShapeDtypeStruct((10, 8, 16), f32),
        in_specs=[pl.BlockSpec(memory_space=pltpu.SMEM)] + [apart] * len(arrays),
        out_specs=pl.BlockSpec(memory_space=VMEM),
        scratch_shapes=[
            VMEM((100, FRAMES, 768), bf16),
            VMEM((100, 1024), bf16),
            VMEM((3, 1024), f32),
            VMEM((1024, 512), bf16),
            *[VMEM(shape, kind) for shape, kind in DENOISER],
            VMEM((8 * KEYS, 1024), bf16),
            VMEM((8, 512), f32),
            VMEM((128, 1536), bf16),
            VMEM((128, 512), bf16),
            VMEM((16, 128), f32),
            VMEM((128, 16), f32),
            VMEM((16, 512), f32),
            VMEM((16, 512), f32),
            VMEM((512, 16), f32),
            VMEM((128, 512), f32),
            VMEM((768, 1024), bf16),
            VMEM((1024, 3072), bf16),
            VMEM((1024, 1024), bf16),
            VMEM((1024, 4096), bf16),
            VMEM((4096, 1024), bf16),
            VMEM((800, 128), f32),
            VMEM((ROWS, 1024), f32),
            VMEM((tall, 1024), f32),
            VMEM((tall, 1024), bf16),
            VMEM((tall, 3072), bf16),
            VMEM((tall, 4096), bf16),
            VMEM((FRAMES * KEYS, 1024), bf16),
            VMEM((FRAMES, KEYS, 512), bf16),
            VMEM((FRAMES, KEYS, 512), bf16),
            pltpu.SemaphoreType.DMA((CHUNKS, LINKS)),
            pltpu.SemaphoreType.DMA((CHUNKS, LINKS)),
            pltpu.SemaphoreType.DMA((CHUNKS,)),
            pltpu.SemaphoreType.DMA((FRAMES,)),
            pltpu.SemaphoreType.DMA((FRAMES,)),
            pltpu.SemaphoreType.DMA((BROUGHT,)),
        ],
        compiler_params=pltpu.CompilerParams(
            vmem_limit_bytes=67043328, collective_id=0, has_side_effects=True
        ),
    )(levels, *arrays)


def on_device(
    pixels,
    patch_weight,
    position,
    encoder_gains,
    qkv_weight,
    out_weight,
    up_weight,
    down_weight,
    cond_weight,
    time_weight,
    action_in,
    action_pos,
    denoise_gains,
    self_qkv,
    self_out,
    cross_query,
    cross_kv,
    cross_out,
    mix_up,
    mix_down,
    action_out,
    noise,
    timesteps,
):
    actions = run_all(
        timesteps,
        jnp.transpose(pixels.reshape(pixels.shape[2:]), (1, 0, 2)),
        patch_weight,
        position,
        encoder_gains,
        qkv_weight,
        out_weight,
        up_weight,
        down_weight,
        cond_weight,
        jnp.transpose(noise.reshape(noise.shape[2:]), (2, 0, 1)),
        time_weight,
        action_in,
        action_pos,
        denoise_gains,
        self_qkv,
        self_out,
        cross_query,
        cross_kv,
        cross_out,
        mix_up,
        mix_down,
        action_out.T,
    )
    return jnp.transpose(actions, (1, 2, 0)).reshape(noise.shape)


def solution(mesh):
    return jax.shard_map(
        on_device,
        mesh=mesh,
        in_specs=(
            P("batch", "mp", None, None, None),
            P("mp", None),
            P(),
            P(),
            P("mp", None),
            P("mp", None),
            P("mp", None),
            P("mp", None),
            P(),
            P(),
            P(),
            P(),
            P(),
            P(),
            P(),
            P(),
            P(),
            P(),
            P(),
            P(),
            P(),
            P("mp", "batch", None, None, None),
            P(),
        ),
        out_specs=P("mp", "batch", None, None, None),
        check_vma=False,
    )
```

```python
import functools
import math

import jax
import jax.numpy as jnp
from jax import lax
from jax.experimental import pallas as pl
from jax.experimental.pallas import tpu as pltpu
from jax.sharding import PartitionSpec as P

GRID = 10
STEPS = 4
TMAX = 100


norm_eps = 1e-06
offset = 0.008


def normalize(values, gain):
    middle = jnp.mean(values, -1, keepdims=True)
    centred = values - middle
    spread = jnp.mean(centred * centred, -1, keepdims=True)
    return centred * lax.rsqrt(spread + norm_eps) * gain


def plan(level):
    angle = (level.astype(jnp.float32) / TMAX + offset) / (1.0 + offset) * (math.pi / 2)
    base = math.cos(offset / (1.0 + offset) * math.pi / 2) ** 2
    return jnp.cos(angle) ** 2 / base


def product(left, right):
    return jnp.dot(left, right, preferred_element_type=jnp.float32)


def precise(left, right):
    return jnp.dot(left, right, precision=lax.Precision.HIGHEST)


VMEM = pltpu.VMEM
KEYS = 32


def stacked_heads(block):
    lane = lax.broadcasted_iota(jnp.int32, block.shape, 1)
    low = jnp.where(lane < 64, block, jnp.zeros_like(block))
    high = jnp.where(lane < 64, jnp.zeros_like(block), block)
    return jnp.concatenate([low, high], axis=0)


def pair_attention(query, keys, values, allowed):
    rows = query.shape[0]
    scores = lax.dot_general(
        stacked_heads(query), keys, (((1,), (1,)), ((), ())), preferred_element_type=jnp.float32
    )
    scores = jnp.where(allowed, scores * (0.125 * math.log2(math.e)), -1e30)
    top = jnp.max(scores, axis=-1, keepdims=True)
    grown = jnp.exp2(scores - top)
    inverse = 1.0 / jnp.sum(grown, axis=-1, keepdims=True)
    probs = (grown * inverse).astype(jnp.bfloat16)
    both = jnp.dot(probs, values, preferred_element_type=jnp.float32)
    lane = lax.broadcasted_iota(jnp.int32, (rows, 128), 1)
    return jnp.where(lane < 64, both[:rows], both[rows:]).astype(jnp.bfloat16)


def gelu(values):
    small = 0.5 * values
    return small + small * lax.erf(values * math.sqrt(0.5))


def denoiser(
    levels_ref,
    condition,
    noise_ref,
    time_ref,
    in_ref,
    pos_ref,
    gains_ref,
    qkv_ref,
    self_out_ref,
    query_ref,
    kv_ref,
    cross_out_ref,
    up_ref,
    down_ref,
    out_ref,
    actions_ref,
    memory,
    stamps,
    packed,
    context,
    flat,
    sample_now,
    widened_in,
    widened_out,
    out_columns,
    held_state,
):
    width = 512
    rows = 128

    def first_half(step):
        own = lax.broadcasted_iota(jnp.int32, (2 * rows, rows), 0)
        other = lax.broadcasted_iota(jnp.int32, (2 * rows, rows), 1)
        same = lax.rem(own, rows) // 16 == other // 16
        state = precise(sample_now[...], widened_in[...])
        state = (state.reshape(8, 16, width) + pos_ref[...]).reshape(rows, width)
        state = state + stamps[pl.ds(step, 1), :]
        normed = normalize(state, gains_ref[0:1, :]).astype(jnp.bfloat16)
        packed[...] = product(normed, qkv_ref[...]).astype(jnp.bfloat16)
        for pair in range(4):
            at = pair * 128
            context[:, at : at + 128] = pair_attention(
                packed[:, at : at + 128],
                packed[:, width + at : width + at + 128],
                packed[:, 2 * width + at : 2 * width + at + 128],
                same,
            )
        state = state + product(context[...], self_out_ref[...])
        held_state[...] = state
        normed = normalize(state, gains_ref[1:2, :]).astype(jnp.bfloat16)
        packed[:, 0:width] = product(normed, query_ref[...]).astype(jnp.bfloat16)

    def begin():
        row = lax.broadcasted_iota(jnp.int32, (8, width // 2), 0)
        level = jnp.zeros((8, width // 2), jnp.float32)
        for step in range(STEPS):
            level = jnp.where(row == step, levels_ref[step].astype(jnp.float32), level)
        order = lax.broadcasted_iota(jnp.int32, (8, width // 2), 1).astype(jnp.float32)
        phase = level * jnp.exp(order * (-math.log(10000.0) / (width // 2)))
        waves = jnp.concatenate([jnp.sin(phase), jnp.cos(phase)], axis=1)
        stamps[...] = precise(waves, time_ref[...])
        for widened, given in ((widened_in, in_ref), (widened_out, out_ref)):
            widened[8:16, :] = jnp.zeros((8, width), jnp.float32)
            widened[0:10, :] = given[...]
        out_columns[...] = widened_out[...].T
        number = lax.broadcasted_iota(jnp.int32, (16, 16), 0)
        for cand in range(8):
            flat[:, cand * 16 : cand * 16 + 16] = jnp.where(number < 10, noise_ref[:, cand, :], 0.0)
        sample_now[...] = flat[...].T
        first_half(0)

    def one_step(step, carry):
        slot = lax.broadcasted_iota(jnp.int32, (2 * rows, 8 * KEYS), 1)
        held = lax.rem(slot, KEYS) < 25
        sample = sample_now[...]
        state = held_state[...]
        for pair in range(4):
            at = pair * 128
            context[:, at : at + 128] = pair_attention(
                packed[:, at : at + 128],
                memory[:, at : at + 128],
                memory[:, width + at : width + at + 128],
                held,
            )
        state = state + product(context[...], cross_out_ref[...])
        normed = normalize(state, gains_ref[2:3, :]).astype(jnp.bfloat16)
        hidden = gelu(product(normed, up_ref[...])).astype(jnp.bfloat16)
        state = state + product(hidden, down_ref[...])
        predicted = precise(state, out_columns[...])
        now = jnp.full((8, 128), levels_ref[step].astype(jnp.float32))
        following = levels_ref[jnp.minimum(step + 1, STEPS - 1)]
        after = plan(jnp.full((8, 128), following.astype(jnp.float32)))
        last = jnp.full((8, 128), step) == STEPS - 1
        after = jnp.where(last, 1.0, after)[0:1, 0:16]
        current = plan(now)[0:1, 0:16]
        clean = (sample - jnp.sqrt(1.0 - current) * predicted) / jnp.sqrt(current)
        sample_now[...] = jnp.sqrt(after) * clean + jnp.sqrt(1.0 - after) * predicted
        pl.when(step < STEPS - 1)(lambda: first_half(step + 1))
        return carry

    def finish():
        memory[...] = product(condition[...].reshape(8 * KEYS, width), kv_ref[...]).astype(
            jnp.bfloat16
        )
        lax.fori_loop(0, STEPS, one_step, 0)
        flat[...] = sample_now[...].T
        for cand in range(8):
            noise_ref[:, cand, :] = flat[:, cand * 16 : cand * 16 + 16]
        actions_ref[...] = noise_ref[0:10]

    return begin, finish


FRAMES = 8
ROWS = 112
LINKS = 24
CHUNKS = 9
MESH = pl.DeviceIdType.MESH
PLAN = {
    "prepare": (
        ("a0", "a1", "a3", "a2",),
        ("o8", "o6", "b0", "o2", "c0", "o0", "b1", "c1", "a4", "b3", "d0", "b2", "o3", "f0", "c2", "c3", "e0", "a5",),
        ("d1", "g0", "e1", "o1", "d2", "h0", "b4", "e2", "c4", "d3", "i0", "o7", "f1", "g1", "f2", "a6", "z0",),
    ),
    "embed": (
        (1, "g2", "e3",),
    ),
    "first_norm": (
        (0, "h1", "g3",),
        (2, "b5", "d4",),
        (3, "c5", "i1",),
        (6, "e4",),
        (7, "h2", "a7", "i2",),
    ),
    "qkv": (
        (0, "z1", "f3",),
        (1, "g4", "i3", "b6", "h3", "f4", "z2", "d5",),
        (2, "f5", "z3", "o4", "a8", "c6", "o5", "e5",),
    ),
    "att": (
        (1, "h4", "g5",),
        (2, "b7", "c7", "d6",),
        (4, "h5", "i4", "f6", "b8",),
        (6, "c8", "e6",),
        (7, "z4", "d7", "i5", "f7", "g6",),
    ),
    "out": (
        (1, "e7",),
    ),
    "second_norm": (
        (0, "d8",),
        (4, "h6",),
        (5, "z5",),
    ),
    "up": (
        (0, "g7", "e8", "i6",),
        (1, "f8",),
        (2, "g8", "z6", "h7",),
        (3, "i7", "h8",),
    ),
    "down": (
        (0, "z7", "i8",),
        (1, "z8",),
    ),
    "tail": (
    ),
}


DENOISER = (
    ((16, 8, 16), jnp.float32),
    ((512, 512), jnp.float32),
    ((10, 512), jnp.float32),
    ((16, 512), jnp.float32),
    ((3, 512), jnp.float32),
    ((512, 1536), jnp.bfloat16),
    ((512, 512), jnp.bfloat16),
    ((512, 512), jnp.bfloat16),
    ((512, 1024), jnp.bfloat16),
    ((512, 512), jnp.bfloat16),
    ((512, 2048), jnp.bfloat16),
    ((2048, 512), jnp.bfloat16),
    ((10, 512), jnp.float32),
)
BROUGHT = len(DENOISER) + 4


def whole_kernel(*refs):
    levels_ref = refs[0]
    given = refs[1 : 10 + len(DENOISER)]
    actions_ref = refs[10 + len(DENOISER)]
    rest = refs[11 + len(DENOISER) :]
    encode_kernel(levels_ref, given, actions_ref, rest[:BROUGHT], rest[BROUGHT : BROUGHT + 10], *rest[BROUGHT + 10 :])


def encode_kernel(
    levels_ref,
    given,
    actions_ref,
    held,
    denoiser_scratch,
    patch_full,
    qkv_full,
    out_full,
    up_full,
    down_full,
    spread,
    place,
    state,
    normed,
    packed,
    hidden,
    pooled,
    leaving,
    landed,
    sent,
    came,
    kept,
    slab_sent,
    slab_came,
    brought,
):
    pixels_in, patch_ref, position_in, gains_in, qkv_ref, out_ref, up_ref, down_ref, cond_in = given[:9]
    pixels_ref, position_ref, gains_ref, cond_ref = held[:4]
    pixels = hidden.at[:, 0:768]
    incoming = (pixels_in, position_in, gains_in, cond_in, *given[9:])

    def bring(i):
        target = held[i].at[0:10] if i == 4 else held[i]
        return pltpu.make_async_copy(incoming[i], target, brought.at[i])

    begin, finish = denoiser(
        levels_ref, landed, *held[4:], actions_ref, *denoiser_scratch
    )
    batch = lax.axis_index("batch")
    part = lax.axis_index("mp")
    near, y = batch // 4, batch % 4
    core = part % 2
    z = (part // 2) % 4
    half = part // 8
    kind = (y + near + half) % 2

    def at_z(by):
        return {"mp": (half * 4 + (z + by) % 4) * 2 + core, "batch": batch}

    def at_y(by):
        return {"batch": near * 4 + (y + by) % 4, "mp": part}

    z_up, z_down, y_up, y_down = at_z(1), at_z(3), at_y(1), at_y(3)
    inner = {"batch": (1 - near) * 4 + y, "mp": part}
    cross = {"batch": (1 - near) * 4 + y, "mp": ((1 - half) * 4 + z) * 2 + core}
    partner = {"batch": batch, "mp": part + 1 - 2 * core}

    chunks = (
        (patch_ref, patch_full, 48, 0, 1024),
        (qkv_ref, qkv_full, 64, 0, 1024),
        (qkv_ref, qkv_full, 64, 1024, 1024),
        (qkv_ref, qkv_full, 64, 2048, 1024),
        (out_ref, out_full, 64, 0, 1024),
        (up_ref, up_full, 64, 0, 2048),
        (up_ref, up_full, 64, 2048, 2048),
        (down_ref, down_full, 256, 0, 512),
        (down_ref, down_full, 256, 512, 512),
    )

    def span(chunk, side, which):
        start, width = chunk[3], chunk[4]
        if which == "all":
            return pl.ds(start, width)
        if which == "half":
            return pl.ds(pl.multiple_of(start + side * (width // 2), 128), width // 2)
        first = start + side * (width // 2) + which * (width // 4)
        return pl.ds(pl.multiple_of(first, 128), width // 4)

    def region(chunk, where, holder, side, which):
        other, by = where
        side_half = 1 - half if other else half
        owner = (side_half * 4 + (z + by) % 4) * 2 + holder
        base = pl.multiple_of(owner * chunk[2], 16)
        return chunk[1].at[pl.ds(base, chunk[2]), span(chunk, side, which)]

    own, below, above, far = (0, 0), (0, 3), (0, 1), (0, 2)
    x_own, x_below, x_above, x_far = (1, 0), (1, 3), (1, 1), (1, 2)
    outgoing = (
        (own, "half", z_up),
        (own, "half", z_down),
        (own, "half", cross),
        (below, 0, z_up),
        (above, 1, z_down),
        (x_own, "half", z_up),
        (x_own, "half", z_down),
        (far, "half", cross),
        (below, "half", y_up),
        (x_below, "half", y_up),
        (x_far, 0, y_up),
        (above, "half", y_down),
        (x_above, "half", y_down),
        (x_far, 1, y_down),
        (x_own, "half", inner),
        (far, "half", inner),
        (own, "all", partner),
        (below, "all", partner),
        (above, "all", partner),
        (x_own, "all", partner),
        (x_below, "all", partner),
        (x_above, "all", partner),
        (far, "all", partner),
        (x_far, "all", partner),
    )
    arriving = (
        (below, "half"),
        (above, "half"),
        (x_own, "half"),
        (far, 0),
        (far, 1),
        (x_below, "half"),
        (x_above, "half"),
        (x_far, "half"),
        (below, "half"),
        (x_below, "half"),
        (x_far, 0),
        (above, "half"),
        (x_above, "half"),
        (x_far, 1),
        (x_own, "half"),
        (far, "half"),
        (own, "all"),
        (below, "all"),
        (above, "all"),
        (x_own, "all"),
        (x_below, "all"),
        (x_above, "all"),
        (far, "all"),
        (x_far, "all"),
    )

    def copy_out(k, slot):
        chunk = chunks[k]
        where, which, peer = outgoing[slot]
        target = region(chunk, where, core, kind, which)
        source = chunk[0].at[:, span(chunk, kind, which)] if where == own else target
        return pltpu.make_async_remote_copy(
            src_ref=source,
            dst_ref=target,
            send_sem=sent.at[k, slot],
            recv_sem=came.at[k, slot],
            device_id=peer,
            device_id_type=MESH,
        )

    def keep(k):
        chunk = chunks[k]
        return pltpu.make_async_copy(
            chunk[0].at[:, span(chunk, 0, "all")], region(chunk, own, core, 0, "all"), kept.at[k]
        )

    def send(k, *slots):
        for slot in slots:
            copy_out(k, slot).start()

    def await_slots(k, *slots):
        for slot in slots:
            where, which = arriving[slot]
            holder = core if slot < 16 else 1 - core
            side = kind if slot < 8 else 1 - kind
            place_here = region(chunks[k], where, holder, side, which)
            pltpu.make_async_remote_copy(
                src_ref=place_here,
                dst_ref=place_here,
                send_sem=sent.at[k, slot],
                recv_sem=came.at[k, slot],
                device_id=partner,
                device_id_type=MESH,
            ).wait_recv()

    moves = {
        "a": ((), (0, 1, 2)),
        "o": ((), (16,)),
        "b": ((0, 1), (3, 4, 8, 11)),
        "c": ((2,), (5, 6, 14)),
        "d": ((3, 4), (7, 15)),
        "e": ((5, 6), (9, 12)),
        "f": ((8, 11, 14), (17, 18, 19)),
        "g": ((7,), (10, 13)),
        "h": ((9, 12, 15), (20, 21, 22)),
        "i": ((10, 13), (23,)),
        "z": ((16, 17, 18, 19, 20, 21, 22, 23), ()),
    }

    def move(names):
        for name in names:
            k = int(name[1])
            awaited, sending = moves[name[0]]
            if name[0] == "o":
                keep(k).start()
            if name[0] == "z":
                keep(k).wait()
            await_slots(k, *awaited)
            send(k, *sending)

    barrier = pltpu.get_barrier_semaphore()
    for peer in (z_up, z_down, cross, partner):
        pl.semaphore_signal(barrier, inc=1, device_id=peer, device_id_type=MESH)
    for by in range(1, FRAMES):
        peer = {"batch": (batch + by) % FRAMES, "mp": part}
        pl.semaphore_signal(barrier, inc=1, device_id=peer, device_id_type=MESH)
    pl.semaphore_wait(barrier, 4 + FRAMES - 1)

    def run(count, body, stage):
        def turn(i, carry):
            for when, *names in PLAN.get(stage, ()):
                pl.when(i == when)(functools.partial(move, names))
            body(i)
            return carry

        lax.fori_loop(0, count, turn, 0)

    def norm_rows(gain):
        def one(i):
            rows = pl.ds(pl.multiple_of(i * ROWS, 16), ROWS)
            normed[rows, :] = normalize(state[rows, :], gains_ref[gain : gain + 1, :]).astype(
                jnp.bfloat16
            )

        return one

    def columns(i, width):
        return pl.ds(pl.multiple_of(i * width, 128), width)

    first, second, third = PLAN["prepare"]
    move(first)
    for i in range(BROUGHT):
        bring(i).start()
    for i in range(BROUGHT):
        bring(i).wait()
    for part_at in range(6):
        lanes = pl.ds(part_at * 128, 128)
        spread[0:800, :] = pixels_ref[:, :, lanes].astype(jnp.float32).reshape(800, 128)
        for frame in range(FRAMES):
            if part_at == 0:
                pixels[frame * ROWS + 96 : (frame + 1) * ROWS, :] = jnp.zeros(
                    (16, 768), jnp.bfloat16
                )
            pixels[frame * ROWS : frame * ROWS + 100, part_at * 128 : part_at * 128 + 128] = spread[
                pl.ds(frame, 100, stride=FRAMES), :
            ].astype(jnp.bfloat16)
    place[96:ROWS, :] = jnp.zeros((16, 1024), jnp.float32)
    place[0:100, :] = position_ref[...].astype(jnp.float32)
    move(second)
    begin()
    move(third)

    def embed(i):
        cols = columns(i, 512)
        raw = product(pixels[...], patch_full[:, cols]).reshape(FRAMES, ROWS, 512)
        state[:, cols] = (raw + place[:, cols]).reshape(FRAMES * ROWS, 512)

    run(2, embed, "embed")
    run(FRAMES, norm_rows(0), "first_norm")

    def pack(i):
        cols = columns(i, 1024)
        packed[:, cols] = product(normed[...], qkv_full[:, cols]).astype(jnp.bfloat16)

    run(3, pack, "qkv")

    key_at = lax.broadcasted_iota(jnp.int32, (2 * ROWS, ROWS), 1)

    def attend(frame):
        rows = pl.ds(pl.multiple_of(frame * ROWS, 16), ROWS)
        for pair in range(8):
            at = pair * 128
            normed[rows, at : at + 128] = pair_attention(
                packed[rows, at : at + 128],
                packed[rows, 1024 + at : 1152 + at],
                packed[rows, 2048 + at : 2176 + at],
                key_at < 100,
            )

    run(FRAMES, attend, "att")

    def project(i):
        rows = pl.ds(pl.multiple_of(i * 448, 16), 448)
        grown = state[rows, :] + product(normed[rows, :], out_full[...])
        state[rows, :] = grown
        normed[rows, :] = normalize(grown, gains_ref[1:2, :]).astype(jnp.bfloat16)

    run(2, project, "out")
    for _, *names in PLAN["second_norm"]:
        move(names)

    def grow(i):
        cols = columns(i, 1024)
        hidden[:, cols] = gelu(product(normed[...], up_full[:, cols])).astype(jnp.bfloat16)

    run(4, grow, "up")

    def shrink(i):
        cols = columns(i, 512)
        state[:, cols] += product(hidden[...], down_full[:, cols])

    run(2, shrink, "down")

    cell = lax.broadcasted_iota(jnp.int32, (KEYS, ROWS), 0)
    patch = lax.broadcasted_iota(jnp.int32, (KEYS, ROWS), 1)
    home = patch // GRID // 2 * (GRID // 2) + patch % GRID // 2
    share = jnp.where((home == cell) & (patch < 100), 0.25, 0.0).astype(jnp.bfloat16)

    def pool(frame):
        rows = pl.ds(pl.multiple_of(frame * ROWS, 16), ROWS)
        final = normalize(state[rows, :], gains_ref[2:3, :])
        high = final.astype(jnp.bfloat16)
        low = (final - high.astype(jnp.float32)).astype(jnp.bfloat16)
        mean = product(share, high) + product(share, low)
        pooled[pl.ds(pl.multiple_of(frame * KEYS, 16), KEYS), :] = mean.astype(jnp.bfloat16)

    run(FRAMES, pool, "tail")
    leaving[...] = (
        product(pooled[...], cond_ref[...]).astype(jnp.bfloat16).reshape(FRAMES, KEYS, 512)
    )

    def slab(by):
        to = (batch + by) % FRAMES
        return pltpu.make_async_remote_copy(
            src_ref=leaving.at[to],
            dst_ref=landed.at[batch],
            send_sem=slab_sent.at[by],
            recv_sem=slab_came.at[by],
            device_id={"batch": to, "mp": part},
            device_id_type=MESH,
        )

    for by in range(1, FRAMES):
        slab(by).start()
    for k in range(CHUNKS):
        for slot in range(LINKS):
            copy_out(k, slot).wait_send()
    landed[batch] = leaving[batch]
    for by in range(1, FRAMES):
        source = (batch + FRAMES - by) % FRAMES
        pltpu.make_async_remote_copy(
            src_ref=landed.at[source],
            dst_ref=landed.at[source],
            send_sem=slab_sent.at[by],
            recv_sem=slab_came.at[by],
            device_id=partner,
            device_id_type=MESH,
        ).wait_recv()
    finish()
    for by in range(1, FRAMES):
        slab(by).wait_send()


def run_all(levels, *arrays):
    bf16, f32 = jnp.bfloat16, jnp.float32
    apart = pl.BlockSpec(memory_space=pl.ANY)
    tall = FRAMES * ROWS
    return pl.pallas_call(
        whole_kernel,
        out_shape=jax.ShapeDtypeStruct((10, 8, 16), f32),
        in_specs=[pl.BlockSpec(memory_space=pltpu.SMEM)] + [apart] * len(arrays),
        out_specs=pl.BlockSpec(memory_space=VMEM),
        scratch_shapes=[
            VMEM((100, FRAMES, 768), bf16),
            VMEM((100, 1024), bf16),
            VMEM((3, 1024), f32),
            VMEM((1024, 512), bf16),
            *[VMEM(shape, kind) for shape, kind in DENOISER],
            VMEM((8 * KEYS, 1024), bf16),
            VMEM((8, 512), f32),
            VMEM((128, 1536), bf16),
            VMEM((128, 512), bf16),
            VMEM((16, 128), f32),
            VMEM((128, 16), f32),
            VMEM((16, 512), f32),
            VMEM((16, 512), f32),
            VMEM((512, 16), f32),
            VMEM((128, 512), f32),
            VMEM((768, 1024), bf16),
            VMEM((1024, 3072), bf16),
            VMEM((1024, 1024), bf16),
            VMEM((1024, 4096), bf16),
            VMEM((4096, 1024), bf16),
            VMEM((832, 128), f32),
            VMEM((ROWS, 1024), f32),
            VMEM((tall, 1024), f32),
            VMEM((tall, 1024), bf16),
            VMEM((tall, 3072), bf16),
            VMEM((tall, 4096), bf16),
            VMEM((FRAMES * KEYS, 1024), bf16),
            VMEM((FRAMES, KEYS, 512), bf16),
            VMEM((FRAMES, KEYS, 512), bf16),
            pltpu.SemaphoreType.DMA((CHUNKS, LINKS)),
            pltpu.SemaphoreType.DMA((CHUNKS, LINKS)),
            pltpu.SemaphoreType.DMA((CHUNKS,)),
            pltpu.SemaphoreType.DMA((FRAMES,)),
            pltpu.SemaphoreType.DMA((FRAMES,)),
            pltpu.SemaphoreType.DMA((BROUGHT,)),
        ],
        compiler_params=pltpu.CompilerParams(
            vmem_limit_bytes=67043328, collective_id=0, has_side_effects=True
        ),
    )(levels, *arrays)


def on_device(
    pixels,
    patch_weight,
    position,
    encoder_gains,
    qkv_weight,
    out_weight,
    up_weight,
    down_weight,
    cond_weight,
    time_weight,
    action_in,
    action_pos,
    denoise_gains,
    self_qkv,
    self_out,
    cross_query,
    cross_kv,
    cross_out,
    mix_up,
    mix_down,
    action_out,
    noise,
    timesteps,
):
    actions = run_all(
        timesteps,
        jnp.transpose(pixels.reshape(pixels.shape[2:]), (1, 0, 2)),
        patch_weight,
        position,
        encoder_gains,
        qkv_weight,
        out_weight,
        up_weight,
        down_weight,
        cond_weight,
        jnp.transpose(noise.reshape(noise.shape[2:]), (2, 0, 1)),
        time_weight,
        action_in,
        action_pos,
        denoise_gains,
        self_qkv,
        self_out,
        cross_query,
        cross_kv,
        cross_out,
        mix_up,
        mix_down,
        action_out.T,
    )
    return jnp.transpose(actions, (1, 2, 0)).reshape(noise.shape)


def solution(mesh):
    return jax.shard_map(
        on_device,
        mesh=mesh,
        in_specs=(
            P("batch", "mp", None, None, None),
            P("mp", None),
            P(),
            P(),
            P("mp", None),
            P("mp", None),
            P("mp", None),
            P("mp", None),
            P(),
            P(),
            P(),
            P(),
            P(),
            P(),
            P(),
            P(),
            P(),
            P(),
            P(),
            P(),
            P(),
            P("mp", "batch", None, None, None),
            P(),
        ),
        out_specs=P("mp", "batch", None, None, None),
        check_vma=False,
    )
```
